32 devices in a mesh: groups: 2 (over x), width: 8 (over z, y), guide: 2 (over core).
Axes of the slice: x: 2, y: 2, z: 4, core: 2. Of those that a mesh axis runs over, the one named last changes fastest.
Arguments:
- latent: float32 [16, 8, 2048], P(None, None, ('groups', 'width')), parts along dimension 2, may hold values from -6 to 6
- starts: int32 [16], P(('groups', 'width')), parts along dimension 0, may hold values from 0 to 1023, as said below
- counts: int32 [2048], P(('groups', 'width')), parts along dimension 0, may hold values from 1 to 3, as said below
- step_index: int32 [2], P('groups'), parts along dimension 0, may hold values from 0 to 27
- cond_mod: float32 [2, 3, 2432], P('guide'), may hold values from -3 to 3
- w_patch: bfloat16 [64, 2432], replicated, may hold values from -0.75 to 0.75
- w_qkv: bfloat16 [2432, 3840], P('width'), may hold values from -0.125 to 0.125
- w_out: bfloat16 [1280, 2432], replicated, may hold values from -0.15625 to 0.15625
- w_final: bfloat16 [2432, 64], replicated, may hold values from -0.125 to 0.125
- w_dec: bfloat16 [144, 512], replicated, may hold values from -0.5 to 0.5
Outputs:
- denoised: float32 [16, 8, 2048], P(None, 'guide', ('groups', 'width')), parts along dimension 2
- features: bfloat16 [8, 2048, 512], P('guide', ('groups', 'width')), parts along dimension 1
The draws below stay inside these ranges and needn't reach their ends.
There are 2 independent parts, one for each index of `groups`. The reference program is written for one: setup_inputs(seed, part) draws one part's arguments, and reference() takes and returns one part's arrays. A program takes and returns all parts, laid end to end along the dimension named above; an argument that names none is the same for every part. Nothing has to cross between parts.
Inputs may be any that keep to these rules, and one draw needn't show every extreme that they name: window k starts between column k * 128 and column (k + 1) * 128 - 1 and covers 2 * 128 columns, wrapping around the panorama. `counts`: the number of windows whose columns, as given by starts, include the column.
All inputs are finite; a program needn't handle non-finite values.
Results may differ from the reference program's by a relative error of at most 0.013.
Values may be sent and summed in bfloat16 or wider, within the bound.
No kernel may reach another device: no remote copies, remote signals or barrier semaphores. Data moves between devices by JAX's collectives and lax.ppermute only.
A program may use at most 128 MiB of HBM per device.

```python
import jax
import jax.numpy as jnp
from jax import lax

D = 2432
HEADS = 20
HEAD = 64
LAT = 16
DEC = 512
STEPS = 28
HL = 8
COLS = 128
WL = 1024
NWIN = 8


def window_begins(key):
    offsets = jax.random.randint(jax.random.fold_in(key, 11), (NWIN,), 0, COLS, dtype=jnp.int32)
    return jnp.arange(NWIN, dtype=jnp.int32) * COLS + offsets


def draw_starts(key, part):
    return window_begins(key)


def draw_counts(key, part):
    begins = window_begins(key)
    columns = jnp.arange(WL, dtype=jnp.int32)
    covered = (columns[None, :] - begins[:, None]) % WL < 2 * COLS
    return jnp.sum(covered.astype(jnp.int32), axis=0).astype(jnp.int32)


def shard_levels(key, shape, shards, low, largest):
    def one(position, blocks):
        heights = jax.random.uniform(jax.random.fold_in(jax.random.fold_in(key, 6), position), (blocks,), jnp.float32, low / len(shards), largest / len(shards))
        return jnp.repeat(jnp.exp(heights), shape[position] // blocks).reshape((-1,) + (1,) * (len(shape) - position - 1))

    gain = one(*shards[0])
    for cut in shards[1:]:
        gain = gain * one(*cut)
    return gain


def gaussian(own_key, shape, scale, most, pieces=(), kind=jnp.bfloat16):
    values = scale * jax.random.normal(own_key, shape, jnp.float32)
    if pieces:
        values = values * shard_levels(own_key, shape, pieces, -0.22, 0.18)
    return jnp.clip(values, -most, most).astype(kind)


def setup_inputs(seed: int = 0, part: int = 0) -> dict:
    arg_keys = jax.random.split(jax.random.key(seed), 11)
    part_splits = jax.random.split(jax.random.fold_in(arg_keys[10], part), 11)
    return {
        "latent": gaussian(part_splits[0], (LAT, HL, WL), 1.0, 6.0, ((2, 8),), jnp.float32),
        "starts": draw_starts(jax.random.fold_in(jax.random.fold_in(arg_keys[10], part), 71), part),
        "counts": draw_counts(jax.random.fold_in(jax.random.fold_in(arg_keys[10], part), 71), part),
        "step_index": jax.random.randint(part_splits[3], (1,), 0, STEPS).astype(jnp.int32),
        "cond_mod": gaussian(arg_keys[4], (2, 3, D), 0.5, 3.0, ((0, 2),), jnp.float32),
        "w_patch": gaussian(arg_keys[5], (4 * LAT, D), (4 * LAT) ** -0.5, 0.75),
        "w_qkv": gaussian(arg_keys[6], (D, 3 * HEADS * HEAD), D ** -0.5, 0.125, ((0, 8),)),
        "w_out": gaussian(arg_keys[7], (HEADS * HEAD, D), (HEADS * HEAD) ** -0.5, 0.15625),
        "w_final": gaussian(arg_keys[8], (D, 4 * LAT), D ** -0.5, 0.125),
        "w_dec": gaussian(arg_keys[9], (9 * LAT, DEC), (9 * LAT) ** -0.5, 0.5),
    }


guidance = 4.0
epsilon = 1e-06

def layer_norm(values):
    centered = values - lax.optimization_barrier(jnp.mean(values, axis=-1, keepdims=True))
    spread = lax.optimization_barrier(jnp.mean(centered * centered, axis=-1, keepdims=True))
    return centered * lax.rsqrt(spread + epsilon)

def head_norm(values):
    return values * lax.rsqrt(lax.optimization_barrier(jnp.mean(values * values, axis=-1, keepdims=True)) + epsilon)

def patchify(window):
    channels, height, breadth = window.shape
    folded = window.reshape(channels, height // 2, 2, breadth // 2, 2).transpose(1, 3, 2, 4, 0)
    return folded.reshape(height // 2 * (breadth // 2), 4 * channels)

def unpatchify(tokens, channels, height, breadth):
    folded = tokens.reshape(height // 2, breadth // 2, 2, 2, channels).transpose(4, 0, 2, 1, 3)
    return folded.reshape(channels, height, breadth)

def attend(queries, key_rows, value_rows):
    scores = jnp.einsum('bqhe,bkhe->bhqk', queries.astype(jnp.float32), key_rows.astype(jnp.float32))
    scores = scores / jnp.sqrt(jnp.float32(queries.shape[-1]))
    weights = jax.nn.softmax(scores, axis=-1).astype(jnp.bfloat16)
    mixed = jnp.einsum('bhqk,bkhe->bqhe', weights.astype(jnp.float32), value_rows.astype(jnp.float32))
    return mixed.astype(jnp.bfloat16)

def convolve(padded, w_dec):
    channels = padded.shape[0]
    height = padded.shape[1] - 2
    breadth = padded.shape[2] - 2
    shifted = [padded[:, row_at:row_at + height, col_at:col_at + breadth] for row_at in range(3) for col_at in range(3)]
    stacked = jnp.stack(shifted).reshape(9 * channels, height * breadth)
    summed = lax.dot_general(stacked, w_dec, (((0,), (0,)), ((), ())), preferred_element_type=jnp.float32)
    return jax.nn.silu(summed).astype(jnp.bfloat16).reshape(height, breadth, w_dec.shape[1])

def branch_velocity(window, modulation, w_patch, w_qkv, w_out, w_final):
    patches = patchify(window)
    token_count = patches.shape[0]
    hidden = jnp.dot(patches, w_patch, preferred_element_type=jnp.float32)
    modulated = (layer_norm(hidden) * (1.0 + modulation[1]) + modulation[0]).astype(jnp.bfloat16)
    projected = jnp.dot(modulated, w_qkv, preferred_element_type=jnp.float32).reshape(token_count, 3, HEADS, HEAD)
    queries = head_norm(projected[:, 0]).astype(jnp.bfloat16)
    key_rows = head_norm(projected[:, 1]).astype(jnp.bfloat16)
    value_rows = projected[:, 2].astype(jnp.bfloat16)
    attended = attend(queries[None], key_rows[None], value_rows[None])[0].reshape(token_count, HEADS * HEAD)
    residual = hidden + modulation[2] * jnp.dot(attended, w_out, preferred_element_type=jnp.float32)
    final_in = layer_norm(residual).astype(jnp.bfloat16)
    result = jnp.dot(final_in, w_final, preferred_element_type=jnp.float32)
    return unpatchify(result, window.shape[0], window.shape[1], window.shape[2])

def reference(latent, starts, counts, step_index, cond_mod, w_patch, w_qkv, w_out, w_final, w_dec):
    fraction = (step_index[0].astype(jnp.float32) + 1.0) / STEPS
    sigma = 3.0 * fraction / (1.0 + 2.0 * fraction)
    total_cols = latent.shape[2]
    rounded = latent.astype(jnp.bfloat16)

    def one_window(summed, begin):
        columns_at = ((begin + jnp.arange(2 * COLS, dtype=jnp.int32)) % total_cols).astype(jnp.int32)
        window = jnp.take(rounded, columns_at, axis=2)
        conditional = branch_velocity(window, cond_mod[0], w_patch, w_qkv, w_out, w_final)
        plain = branch_velocity(window, cond_mod[1], w_patch, w_qkv, w_out, w_final)
        guided = plain + guidance * (conditional - plain)
        return (summed.at[:, :, columns_at].add(guided), None)
    summed, unused = lax.scan(one_window, jnp.zeros(latent.shape, jnp.float32), starts)
    velocity = summed / counts.astype(jnp.float32)[None, None, :]
    denoised = latent - sigma * velocity
    padded = jnp.pad(denoised.astype(jnp.bfloat16), ((0, 0), (1, 1), (1, 1)))
    features = convolve(padded, w_dec)
    return (denoised, features)
```

```python
import functools

import jax
import jax.numpy as jnp
from jax import lax
from jax.experimental import pallas as pl
from jax.experimental.pallas import tpu as pltpu
from jax.sharding import PartitionSpec as P

HEADS = 20
HEAD = 64
STEPS = 28
LANES = 128
ROWS = 72

guidance = 4.0
epsilon = 1e-06

bf16 = jnp.bfloat16
f32 = jnp.float32
PARTS = (0, 2, 1)
LOG2E = 1.4426950408889634


def dot(a, b, dims=((1,), (0,))):
    return lax.dot_general(a, b, (dims, ((), ())), preferred_element_type=f32)


def call(body, outs, scratch=(), anys=(), smem=(), count=0, limit=56):
    def spec(i):
        if i in anys:
            return pl.BlockSpec(memory_space=pl.ANY)
        if i in smem:
            return pl.BlockSpec(memory_space=pltpu.SMEM)
        return pl.BlockSpec(memory_space=pltpu.VMEM)

    return pl.pallas_call(
        body,
        out_shape=tuple(jax.ShapeDtypeStruct(s, t) for s, t in outs),
        in_specs=[spec(i) for i in range(count)],
        out_specs=tuple(pl.BlockSpec(memory_space=pltpu.VMEM) for _ in outs),
        scratch_shapes=list(scratch),
        compiler_params=pltpu.CompilerParams(vmem_limit_bytes=limit << 20),
    )


def iota(shape, dim):
    return lax.broadcasted_iota(jnp.int32, shape, dim)


def split(values):
    high = values.astype(bf16)
    return high, (values - high.astype(f32)).astype(bf16)


def partial_kernel(place_ref, a_ref, w_ref, out_ref, w_buf, sems, *, width, slots, local_pairs, features):
    group = place_ref[0]
    span = local_pairs * LANES
    copies = []
    for part in range(3):
        start = pl.multiple_of(part * features + group * span, LANES)
        copies.append(
            pltpu.make_async_copy(w_ref.at[:, pl.ds(start, span)], w_buf.at[part], sems.at[part])
        )
    for one in copies:
        one.start()
    for one in copies:
        one.wait()
    a = a_ref[...]
    for owner in range(width):
        for slot in range(slots):
            tile = owner * slots + slot
            if tile < 3 * local_pairs:
                pair, sub = divmod(tile, 3)
                both = dot(a, w_buf[PARTS[sub], :, pair * LANES : (pair + 1) * LANES])
                value = (both[:ROWS] + both[ROWS:]).astype(bf16)
            else:
                value = jnp.zeros((ROWS, LANES), bf16)
            out_ref[owner, :, slot * LANES : (slot + 1) * LANES] = value


def sum_kernel(parts_ref, out_ref, *, width):
    total = parts_ref[0].astype(f32)
    for i in range(1, width):
        total = total + parts_ref[i].astype(f32)
    out_ref[...] = total.astype(bf16)


def window_kernel(
    place_ref, own_ref, right_ref, left_ref, further_ref, w_ref,
    x_ref, xt_ref, var_ref, varrow_ref, lat_ref, count_ref,
    rows_buf, xt_buf, hid_buf,
):
    channels, height, columns = own_ref.shape[0] - 1, own_ref.shape[1], own_ref.shape[2]
    offset = place_ref[1]
    guide = place_ref[2]
    near = height // 2 + 1
    lane = iota((channels, LANES), 1)
    for r in range(height):
        at = slice(r * channels, (r + 1) * channels)
        rows_buf[at, :columns] = own_ref[:channels, r, :].astype(bf16)
        rows_buf[at, columns : 2 * columns] = right_ref[:channels, r, :].astype(bf16)
        rows_buf[at, 2 * columns :] = further_ref[:, r, :]
    col = iota((3 * columns, 2 * columns), 0)
    spot = iota((3 * columns, 2 * columns), 1)
    b = (spot >= columns).astype(jnp.int32)
    pick = jnp.where(col == offset + 2 * (spot - b * columns) + b, 1.0, 0.0).astype(bf16)
    placed = dot(rows_buf[...], pick).astype(bf16)
    tokens = height // 2 * columns
    for p in range(height // 2):
        for a in range(2):
            for b in range(2):
                f = (a * 2 + b) * channels
                xt_buf[f : f + channels, p * columns : (p + 1) * columns] = placed[
                    (2 * p + a) * channels : (2 * p + a + 1) * channels, b * columns : (b + 1) * columns
                ].astype(f32)
    feats = 4 * channels
    xt = xt_buf[:feats, :]
    xpad = jnp.concatenate([xt, jnp.zeros((LANES - feats, tokens), f32)], axis=0)
    xrow = xpad.T
    model = w_ref.shape[1]
    block = 64
    x_bf = xrow[:, :feats].astype(bf16)
    hid_buf[...] = dot(x_bf, w_ref[...])

    def stats(i, carry):
        at = pl.ds(pl.multiple_of(i * block, block), block)
        h = hid_buf[at, :]
        mean = jnp.sum(h, axis=1, keepdims=True) * (1.0 / model)
        c = h - mean
        v = jnp.sum(c * c, axis=1, keepdims=True) * (1.0 / model)
        var_ref[at, :] = jnp.broadcast_to(v, (block, LANES))
        return carry

    lax.fori_loop(0, tokens // block, stats, 0)
    var = var_ref[...]
    std_hi, std_lo = split(jnp.sqrt(var + epsilon))
    spots = iota((tokens, LANES), 1)
    x_ref[...] = jnp.where(
        spots == feats, std_hi.astype(f32), jnp.where(spots == feats + 1, std_lo.astype(f32), xrow)
    ).astype(bf16)
    var_t = var.T[:8]
    varrow_ref[...] = var_t
    hi_t, lo_t = split(jnp.sqrt(var_t + epsilon))
    down = iota((8, tokens), 0)
    tail = jnp.where(down == 0, hi_t.astype(f32), jnp.where(down == 1, lo_t.astype(f32), 0.0))
    xt_ref[...] = jnp.concatenate([xt, tail], axis=0).astype(bf16)
    first = guide * (near - 2)
    for i in range(near):
        r = pl.ds(first + i, 1)
        lat_ref[i, :, :columns] = own_ref[:channels, r, :].reshape(channels, columns)
        before = pltpu.roll(left_ref[:channels, r, :].reshape(channels, columns), 1, 1)
        after = pltpu.roll(right_ref[:channels, r, :].reshape(channels, columns), 1, 1)
        lat_ref[i, :, columns:] = jnp.where(lane == 0, before, jnp.where(lane == 1, after, 0.0))
    lane8 = iota((height, LANES), 1)
    count_ref[:, :columns] = own_ref[channels]
    before = pltpu.roll(left_ref[channels], 1, 1)
    after = pltpu.roll(right_ref[channels], 1, 1)
    count_ref[:, columns:] = jnp.where(lane8 == 0, before, jnp.where(lane8 == 1, after, 1.0))


def attend_pairs(m_ref, x_ref, xt_ref, var_ref, varrow_ref, att_ref, slots, pairs):
    tokens = x_ref.shape[0]
    x = x_ref[:, :ROWS]
    xt = xt_ref[...]
    var = var_ref[...]
    eps_col = epsilon * (var + epsilon)
    rstd = lax.rsqrt(var + epsilon)
    eps_row = epsilon * (varrow_ref[:1, :] + epsilon)
    low = iota((tokens, LANES), 1) < HEAD
    scale = LOG2E * HEAD**-0.5

    def tile(t):
        slot = t % slots
        return m_ref[t // slots, :, slot * LANES : (slot + 1) * LANES]

    for pair in range(pairs):
        mq, mv, mk = (tile(3 * pair + sub) for sub in range(3))
        both = dot(x, jnp.concatenate([mq, mv], axis=1))
        uq = both[:, :LANES]
        uv = both[:, LANES:] * rstd
        uk = dot(mk, xt, ((0,), (0,)))
        sq = uq * uq
        sum_low = jnp.sum(jnp.where(low, sq, 0.0), axis=1, keepdims=True)
        sum_high = jnp.sum(jnp.where(low, 0.0, sq), axis=1, keepdims=True)
        q = uq * lax.rsqrt(jnp.where(low, sum_low, sum_high) * (1.0 / HEAD) + eps_col)
        keys = []
        for half in range(2):
            k = uk[half * HEAD : (half + 1) * HEAD]
            mean = jnp.sum(k * k, axis=0, keepdims=True) * (1.0 / HEAD)
            keys.append((k * lax.rsqrt(mean + eps_row)).astype(bf16))
        kt = jnp.concatenate(keys, axis=0)
        outs = []
        for half in range(2):
            mine = low if half == 0 else jnp.logical_not(low)
            qh = jnp.where(mine, q, 0.0).astype(bf16)
            vh = jnp.where(mine, uv, 1.0).astype(bf16)
            weights = jnp.exp2(dot(qh, kt) * scale).astype(bf16)
            outs.append(dot(weights, vh))
        top = jnp.where(low, outs[0], outs[1])
        sums = pltpu.roll(jnp.where(low, outs[1], outs[0]), HEAD, 1)
        att_ref[:, pair * LANES : (pair + 1) * LANES] = (top / sums).astype(bf16)


def first_kernel(m_ref, x_ref, xt_ref, var_ref, varrow_ref, att_ref, *, slots, pairs):
    attend_pairs(m_ref, x_ref, xt_ref, var_ref, varrow_ref, att_ref, slots, pairs)


def second_kernel(
    place_ref, m_ref, x_ref, xt_ref, var_ref, varrow_ref, att_ref, wp_ref, gate_ref, wf_ref, wo_ref,
    mine_ref, send_ref,
    att_buf, wo_buf, res_buf, fin_buf, sem,
    *, slots, pairs, channels, height, columns, halves,
):
    load = pltpu.make_async_copy(wo_ref, wo_buf, sem.at[0])
    load.start()
    group = place_ref[0]
    guide = place_ref[2]
    attend_pairs(m_ref, x_ref, xt_ref, var_ref, varrow_ref, att_buf, slots, pairs) if halves == 2 else None
    load.wait()
    tokens = x_ref.shape[0]
    feats = wp_ref.shape[0]
    model = wp_ref.shape[1]
    span = pairs * LANES
    x = x_ref[:, :feats]
    first = pl.multiple_of(group * span, LANES) if halves == 2 else 0
    other = pl.multiple_of((1 - group) * span, LANES)
    start = 0
    while start < model:
        size = min(2 * LANES, model - start)
        cols = slice(start, start + size)
        mixed = dot(att_ref[...], wo_buf[pl.ds(first, span), cols])
        if halves == 2:
            mixed = mixed + dot(att_buf[...], wo_buf[pl.ds(other, span), cols])
        res_buf[:, cols] = dot(x, wp_ref[:, cols]) + gate_ref[:, cols] * mixed
        start += size
    block = 32

    def norm(i, carry):
        at = pl.ds(pl.multiple_of(i * block, block), block)
        h = res_buf[at, :]
        mean = jnp.sum(h, axis=1, keepdims=True) * (1.0 / model)
        c = h - mean
        v = jnp.sum(c * c, axis=1, keepdims=True) * (1.0 / model)
        fin_buf[at, :] = (c * lax.rsqrt(v + epsilon)).astype(bf16)
        return carry

    lax.fori_loop(0, tokens // block, norm, 0)
    result = dot(fin_buf[...], wf_ref[...])
    near = height // 2 + 1
    keep = guide * (near - 2)
    give = (1 - guide) * (near - 2)
    for p in range(height // 2):
        turned = result[p * columns : (p + 1) * columns].T
        for a in range(2):
            r = 2 * p + a
            for b in range(2):
                f = (a * 2 + b) * channels
                piece = turned[f : f + channels]

                @pl.when(jnp.logical_and(r >= keep, r < keep + near))
                def _():
                    mine_ref[r - keep, :, b * columns : (b + 1) * columns] = piece

                @pl.when(jnp.logical_and(r >= give, r < give + near))
                def _():
                    send_ref[r - give, :, b * columns : (b + 1) * columns] = piece.astype(bf16)


def spread_kernel(place_ref, mine_ref, theirs_ref, own_ref, one_ref, two_ref, back_ref):
    offset = place_ref[1]
    guide = place_ref[2]
    near, channels, wide = mine_ref.shape
    columns = wide // 2
    mine = mine_ref[...].reshape(near * channels, wide)
    theirs = theirs_ref[...].reshape(near * channels, wide).astype(f32)
    cond = jnp.where(guide == 0, mine, theirs)
    plain = jnp.where(guide == 0, theirs, mine)
    guided = plain + guidance * (cond - plain)
    high, low = split(guided)
    spot = iota((wide, 2 * columns), 0)
    lane = iota((wide, 2 * columns), 1)
    b = (spot >= columns).astype(jnp.int32)
    col = offset + 2 * (spot - b * columns) + b
    target = jnp.where(lane < columns, lane, jnp.where(lane == columns, -1, lane - 1))
    target = jnp.where(lane > columns + 1, -4 * wide, target)

    def place(distance):
        return jnp.where(col == target + distance * columns, 1.0, 0.0).astype(bf16)

    here = place(0)
    own_ref[...] = dot(high, here) + dot(low, here)
    one_ref[...] = dot(high, place(1)).astype(bf16)
    two_ref[...] = dot(high, place(2)).astype(bf16)
    back_ref[...] = dot(high, place(-1)[:, columns:]).astype(bf16)


def decode_kernel(
    place_ref, own_ref, one_ref, two_ref, back_ref, lat_ref, count_ref, w_ref, den_ref, feat_ref, pad_buf,
    *, width,
):
    guide = place_ref[2]
    place = place_ref[3]
    near, channels, wide = lat_ref.shape
    columns = wide // 2
    fraction = (jnp.full((1, wide), place_ref[4], jnp.int32).astype(f32) + 1.0) / STEPS
    sigma = 3.0 * fraction / (1.0 + 2.0 * fraction)
    total = own_ref[...] + one_ref[...].astype(f32) + two_ref[...].astype(f32)
    back = jnp.concatenate([jnp.zeros(back_ref.shape, f32), back_ref[...].astype(f32)], axis=1)
    velocity = (total + back) / count_ref[:1, :]
    clean = lat_ref[...].reshape(near * channels, wide) - sigma * velocity
    half = near - 1
    first = guide
    lane = iota((near * channels, columns), 1)
    main = clean[:, :columns]
    edges = clean[:, columns:]
    left = jnp.where(place == 0, 0.0, edges[:, 0:1])
    right = jnp.where(place == width - 1, 0.0, edges[:, 1:2])
    before = jnp.where(lane == 0, left, pltpu.roll(main, 1, 1))
    after = jnp.where(lane == columns - 1, right, pltpu.roll(main, columns - 1, 1))
    zero = jnp.zeros((channels, columns), f32)
    for b, value in enumerate((before, main, after)):
        pad_buf[b, 0] = zero
        pad_buf[b, near + 1] = zero
        for i in range(near):
            pad_buf[b, i + 1] = value[i * channels : (i + 1) * channels]
    for r in range(half):
        at = first + r
        den_ref[:, r, :] = pad_buf[1, at + 1]
        stacked = jnp.concatenate(
            [pad_buf[b, at + a] for a in range(3) for b in range(3)], axis=0
        ).astype(bf16)
        summed = dot(stacked, w_ref[...], ((0,), (0,)))
        feat_ref[r] = (summed / (1.0 + jnp.exp(-summed))).astype(bf16)


def shift(x, by):
    peers = lax.axis_size("width")
    return lax.ppermute(x, "width", [(i, (i + by) % peers) for i in range(peers)])


def swap(x, axis):
    return lax.ppermute(x, axis, [(0, 1), (1, 0)])


def shards(latent, starts, counts, step_index, cond_mod, w_patch, w_qkv, w_out, w_final, w_dec):
    guide = lax.axis_index("guide")
    place = lax.axis_index("width")
    group = lax.axis_index("groups")
    width = lax.axis_size("width")
    channels, height, columns = latent.shape
    model = w_patch.shape[1]
    feats = w_patch.shape[0]
    features = HEADS * HEAD
    pairs = features // LANES
    halves = 2 if lax.axis_size("groups") == 2 and pairs % 2 == 0 else 1
    local_pairs = pairs // halves
    slots = -(-3 * local_pairs // width)
    if halves == 1:
        group = group * 0
    rows = w_qkv.shape[0]
    modulation = cond_mod[0]
    offset = starts[0] - place * columns
    scalars = jnp.stack([group, offset, guide, place, step_index[0]]).astype(jnp.int32)

    pack = jnp.concatenate(
        [latent, jnp.broadcast_to(counts.astype(f32)[None, None, :], (1, height, columns))], axis=0
    )
    right = shift(pack, -1)
    further = shift(latent.astype(bf16), -2)
    left = shift(pack, 1)

    wide = w_patch.astype(f32)
    centered = wide - jnp.mean(wide, axis=1, keepdims=True)
    mine = lax.dynamic_slice_in_dim(centered, place * rows, rows, 1)
    own_mod = lax.dynamic_slice_in_dim(modulation, place * rows, rows, 1)
    shift_rows = jnp.concatenate([own_mod[0:1]] * 2 + [jnp.zeros((ROWS - feats - 2, rows), f32)])
    stacked = jnp.concatenate([mine * (1.0 + own_mod[1:2]), shift_rows])
    a = jnp.concatenate(split(stacked), axis=0)

    (parts,) = call(
        functools.partial(
            partial_kernel, width=width, slots=slots, local_pairs=local_pairs, features=features
        ),
        [((width, ROWS, slots * LANES), bf16)],
        scratch=[
            pltpu.VMEM((3, rows, local_pairs * LANES), bf16),
            pltpu.SemaphoreType.DMA((3,)),
        ],
        anys=(2,), smem=(0,), count=3,
    )(scalars, a, w_qkv)
    parts = lax.all_to_all(parts, "width", 0, 0, tiled=True)
    (chunk,) = call(
        functools.partial(sum_kernel, width=width), [((ROWS, slots * LANES), bf16)], count=1
    )(parts)
    near = height // 2 + 1
    tokens = height // 2 * columns
    x, xt, var, varrow, lat, count = call(
        window_kernel,
        [
            ((tokens, LANES), bf16), ((ROWS, tokens), bf16), ((tokens, LANES), f32),
            ((8, tokens), f32), ((near, channels, 2 * columns), f32), ((height, 2 * columns), f32),
        ],
        scratch=[
            pltpu.VMEM((height * channels, 3 * columns), bf16),
            pltpu.VMEM((feats, tokens), f32),
            pltpu.VMEM((tokens, model), f32),
        ],
        smem=(0,), count=6,
    )(scalars, pack, right, left, further, w_patch)
    half = lax.all_to_all(
        jnp.broadcast_to(chunk[None], (width,) + chunk.shape), "width", 0, 0, tiled=True
    )
    other = swap(half, "groups") if halves == 2 else half
    (att,) = call(
        functools.partial(first_kernel, slots=slots, pairs=local_pairs),
        [((tokens, local_pairs * LANES), bf16)],
        count=5,
    )(half, x, xt, var, varrow)
    mine_v, send_v = call(
        functools.partial(
            second_kernel, slots=slots, pairs=local_pairs, channels=channels, height=height,
            columns=columns, halves=halves,
        ),
        [((near, channels, 2 * columns), f32), ((near, channels, 2 * columns), bf16)],
        scratch=[
            pltpu.VMEM((tokens, local_pairs * LANES), bf16),
            pltpu.VMEM(w_out.shape, bf16),
            pltpu.VMEM((tokens, model), f32),
            pltpu.VMEM((tokens, model), bf16),
            pltpu.SemaphoreType.DMA((1,)),
        ],
        anys=(10,), smem=(0,), count=11,
    )(scalars, other, x, xt, var, varrow, att, w_patch, modulation[2:3], w_final, w_out)
    theirs = swap(send_v, "guide")
    flat = near * channels
    own, one, two, back = call(
        spread_kernel,
        [
            ((flat, 2 * columns), f32), ((flat, 2 * columns), bf16),
            ((flat, 2 * columns), bf16), ((flat, columns), bf16),
        ],
        smem=(0,), count=3,
    )(scalars, mine_v, theirs)
    one = shift(one, 1)
    two = shift(two, 2)
    back = shift(back, -1)
    return call(
        functools.partial(decode_kernel, width=width),
        [((channels, height // 2, columns), f32), ((height // 2, columns, w_dec.shape[1]), bf16)],
        scratch=[pltpu.VMEM((3, near + 2, channels, columns), f32)],
        smem=(0,), count=8,
    )(scalars, own, one, two, back, lat, count, w_dec)


def solution(mesh):
    return jax.shard_map(
        shards,
        mesh=mesh,
        in_specs=(
            P(None, None, ("groups", "width")),
            P(("groups", "width")),
            P(("groups", "width")),
            P("groups"),
            P("guide", None, None),
            P(),
            P("width", None),
            P(),
            P(),
            P(),
        ),
        out_specs=(P(None, "guide", ("groups", "width")), P("guide", ("groups", "width"), None)),
        check_vma=False,
    )
```

```python
import functools

import jax
import jax.numpy as jnp
from jax import lax
from jax.experimental import pallas as pl
from jax.experimental.pallas import tpu as pltpu
from jax.sharding import PartitionSpec as P

HEADS = 20
HEAD = 64
STEPS = 28
LANES = 128
ROWS = 72

guidance = 4.0
epsilon = 1e-06

bf16 = jnp.bfloat16
f32 = jnp.float32
PARTS = (0, 2, 1)
LOG2E = 1.4426950408889634


def dot(a, b, dims=((1,), (0,))):
    return lax.dot_general(a, b, (dims, ((), ())), preferred_element_type=f32)


def call(body, outs, scratch=(), anys=(), smem=(), count=0, limit=56, flops=0):
    def spec(i):
        if i in anys:
            return pl.BlockSpec(memory_space=pl.ANY)
        if i in smem:
            return pl.BlockSpec(memory_space=pltpu.SMEM)
        return pl.BlockSpec(memory_space=pltpu.VMEM)

    return pl.pallas_call(
        body,
        out_shape=tuple(jax.ShapeDtypeStruct(s, t) for s, t in outs),
        in_specs=[spec(i) for i in range(count)],
        out_specs=tuple(pl.BlockSpec(memory_space=pltpu.VMEM) for _ in outs),
        scratch_shapes=list(scratch),
        compiler_params=pltpu.CompilerParams(vmem_limit_bytes=limit << 20),
        cost_estimate=pl.CostEstimate(flops=int(flops), bytes_accessed=1 << 20, transcendentals=0),
    )


def iota(shape, dim):
    return lax.broadcasted_iota(jnp.int32, shape, dim)


def split(values):
    high = values.astype(bf16)
    return high, (values - high.astype(f32)).astype(bf16)


def partial_kernel(
    place_ref, mod_ref, wp_ref, w_ref, out_ref, w_buf, sems, *, width, slots, local_pairs, features
):
    group = place_ref[0]
    span = local_pairs * LANES
    copies = []
    for part in range(3):
        start = pl.multiple_of(part * features + group * span, LANES)
        copies.append(
            pltpu.make_async_copy(w_ref.at[:, pl.ds(start, span)], w_buf.at[part], sems.at[part])
        )
    for one in copies:
        one.start()
    feats, model = wp_ref.shape
    rows = w_buf.shape[1]
    window = min(model, -(-(rows + LANES - 1) // LANES) * LANES)
    begin = place_ref[3] * rows
    low = jnp.minimum(begin // LANES * LANES, model - window)
    cols = pl.ds(pl.multiple_of(low, LANES), window)
    mean = jnp.sum(wp_ref[...].astype(f32), axis=1, keepdims=True) * (1.0 / model)
    centered = wp_ref[:, cols].astype(f32) - mean
    scaled = centered * (1.0 + mod_ref[0, 1:2, cols])
    down = iota((ROWS - feats, window), 0)
    tail = jnp.where(down < 2, jnp.broadcast_to(mod_ref[0, 0:1, cols], down.shape), 0.0)
    stacked = jnp.concatenate([scaled, tail], axis=0)
    stacked = pltpu.roll(stacked, (window - (begin - low)) % window, 1)
    a = jnp.concatenate(split(stacked), axis=0)[:, :rows]
    for one in copies:
        one.wait()
    for owner in range(width):
        for slot in range(slots):
            tile = owner * slots + slot
            if tile < 3 * local_pairs:
                pair, sub = divmod(tile, 3)
                both = dot(a, w_buf[PARTS[sub], :, pair * LANES : (pair + 1) * LANES])
                value = (both[:ROWS] + both[ROWS:]).astype(bf16)
            else:
                value = jnp.zeros((ROWS, LANES), bf16)
            out_ref[owner, :, slot * LANES : (slot + 1) * LANES] = value


def sum_kernel(parts_ref, out_ref, *, width):
    total = parts_ref[0].astype(f32)
    for i in range(1, width):
        total = total + parts_ref[i].astype(f32)
    out_ref[...] = total.astype(bf16)


def window_kernel(
    place_ref, own_ref, right_ref, left_ref, further_ref, w_ref,
    x_ref, xt_ref, var_ref, varrow_ref, lat_ref, count_ref,
    rows_buf, xt_buf, hid_buf,
):
    channels, height, columns = own_ref.shape[0] - 1, own_ref.shape[1], own_ref.shape[2]
    offset = place_ref[1]
    guide = place_ref[2]
    near = height // 2 + 1
    lane = iota((channels, LANES), 1)
    for r in range(height):
        at = slice(r * channels, (r + 1) * channels)
        rows_buf[at, :columns] = own_ref[:channels, r, :].astype(bf16)
        rows_buf[at, columns : 2 * columns] = right_ref[:channels, r, :].astype(bf16)
        rows_buf[at, 2 * columns :] = further_ref[:, r, :]
    col = iota((3 * columns, 2 * columns), 0)
    spot = iota((3 * columns, 2 * columns), 1)
    b = (spot >= columns).astype(jnp.int32)
    pick = jnp.where(col == offset + 2 * (spot - b * columns) + b, 1.0, 0.0).astype(bf16)
    placed = dot(rows_buf[...], pick).astype(bf16)
    tokens = height // 2 * columns
    for p in range(height // 2):
        for a in range(2):
            for b in range(2):
                f = (a * 2 + b) * channels
                xt_buf[f : f + channels, p * columns : (p + 1) * columns] = placed[
                    (2 * p + a) * channels : (2 * p + a + 1) * channels, b * columns : (b + 1) * columns
                ].astype(f32)
    feats = 4 * channels
    xt = xt_buf[:feats, :]
    xpad = jnp.concatenate([xt, jnp.zeros((LANES - feats, tokens), f32)], axis=0)
    xrow = xpad.T
    model = w_ref.shape[1]
    block = 64
    x_bf = xrow[:, :feats].astype(bf16)
    hid_buf[...] = dot(x_bf, w_ref[...])

    def stats(i, carry):
        at = pl.ds(pl.multiple_of(i * block, block), block)
        h = hid_buf[at, :]
        mean = jnp.sum(h, axis=1, keepdims=True) * (1.0 / model)
        c = h - mean
        v = jnp.sum(c * c, axis=1, keepdims=True) * (1.0 / model)
        var_ref[at, :] = jnp.broadcast_to(v, (block, LANES))
        return carry

    lax.fori_loop(0, tokens // block, stats, 0)
    var = var_ref[...]
    std_hi, std_lo = split(jnp.sqrt(var + epsilon))
    spots = iota((tokens, LANES), 1)
    x_ref[...] = jnp.where(
        spots == feats, std_hi.astype(f32), jnp.where(spots == feats + 1, std_lo.astype(f32), xrow)
    ).astype(bf16)
    var_t = var.T[:8]
    varrow_ref[...] = var_t
    hi_t, lo_t = split(jnp.sqrt(var_t + epsilon))
    down = iota((8, tokens), 0)
    tail = jnp.where(down == 0, hi_t.astype(f32), jnp.where(down == 1, lo_t.astype(f32), 0.0))
    xt_ref[...] = jnp.concatenate([xt, tail], axis=0).astype(bf16)
    first = guide * (near - 2)
    for i in range(near):
        r = pl.ds(first + i, 1)
        lat_ref[i, :, :columns] = own_ref[:channels, r, :].reshape(channels, columns)
        before = pltpu.roll(left_ref[:channels, r, :].reshape(channels, columns), 1, 1)
        after = pltpu.roll(right_ref[:channels, r, :].reshape(channels, columns), 1, 1)
        lat_ref[i, :, columns:] = jnp.where(lane == 0, before, jnp.where(lane == 1, after, 0.0))
    lane8 = iota((height, LANES), 1)
    count_ref[:, :columns] = own_ref[channels]
    before = pltpu.roll(left_ref[channels], 1, 1)
    after = pltpu.roll(right_ref[channels], 1, 1)
    count_ref[:, columns:] = jnp.where(lane8 == 0, before, jnp.where(lane8 == 1, after, 1.0))


def attend_pairs(place_ref, near_ref, far_ref, x_ref, xt_ref, var_ref, varrow_ref, put, slots, pairs, fold):
    tokens = x_ref.shape[0]
    key = place_ref[5]
    side = place_ref[3] % fold
    x = x_ref[:, :ROWS]
    xt = xt_ref[...]
    var = var_ref[...]
    eps_col = epsilon * (var + epsilon)
    rstd = lax.rsqrt(var + epsilon)
    eps_row = epsilon * (varrow_ref[:1, :] + epsilon)
    low = iota((tokens, LANES), 1) < HEAD
    scale = LOG2E * HEAD**-0.5

    def tile(t):
        owner, slot = divmod(t, slots)
        z, y = divmod(owner, fold)
        at = (z ^ key, slice(None), slice(slot * LANES, (slot + 1) * LANES))
        return jnp.where(side == y, near_ref[at], far_ref[at])

    for pair in range(pairs):
        mq, mv, mk = (tile(3 * pair + sub) for sub in range(3))
        both = dot(x, jnp.concatenate([mq, mv], axis=1))
        uq = both[:, :LANES]
        uv = both[:, LANES:] * rstd
        uk = dot(mk, xt, ((0,), (0,)))
        sq = uq * uq
        sum_low = jnp.sum(jnp.where(low, sq, 0.0), axis=1, keepdims=True)
        sum_high = jnp.sum(jnp.where(low, 0.0, sq), axis=1, keepdims=True)
        q = uq * lax.rsqrt(jnp.where(low, sum_low, sum_high) * (1.0 / HEAD) + eps_col)
        keys = []
        for half in range(2):
            k = uk[half * HEAD : (half + 1) * HEAD]
            mean = jnp.sum(k * k, axis=0, keepdims=True) * (1.0 / HEAD)
            keys.append((k * lax.rsqrt(mean + eps_row)).astype(bf16))
        kt = jnp.concatenate(keys, axis=0)
        outs = []
        for half in range(2):
            mine = low if half == 0 else jnp.logical_not(low)
            qh = jnp.where(mine, q, 0.0).astype(bf16)
            vh = jnp.where(mine, uv, 1.0).astype(bf16)
            weights = jnp.exp2(dot(qh, kt) * scale).astype(bf16)
            outs.append(dot(weights, vh))
        top = jnp.where(low, outs[0], outs[1])
        sums = pltpu.roll(jnp.where(low, outs[1], outs[0]), HEAD, 1)
        put(pair, (top / sums).astype(bf16))


def first_kernel(
    place_ref, near_ref, far_ref, x_ref, xt_ref, var_ref, varrow_ref, att_ref, *, slots, pairs, fold
):
    def put(pair, value):
        att_ref[:, pair * LANES : (pair + 1) * LANES] = value

    attend_pairs(place_ref, near_ref, far_ref, x_ref, xt_ref, var_ref, varrow_ref, put, slots, pairs, fold)


def second_kernel(
    place_ref, near_ref, far_ref, x_ref, xt_ref, var_ref, varrow_ref, att_ref, wp_ref, mod_ref, wf_ref, wo_ref,
    mine_ref, send_ref,
    att_buf, wo_buf, res_buf, fin_buf, sum_buf, sem,
    *, slots, pairs, channels, height, columns, halves, fold,
):
    load = pltpu.make_async_copy(wo_ref, wo_buf, sem.at[0])
    load.start()
    group = place_ref[0]
    guide = place_ref[2]
    span = pairs * LANES
    first = pl.multiple_of(group * span, LANES) if halves == 2 else 0
    att_buf[:, pl.ds(first, span)] = att_ref[...]
    if halves == 2:
        other = (1 - group) * span

        def put(pair, value):
            at = pl.multiple_of(other + pair * LANES, LANES)
            att_buf[:, pl.ds(at, LANES)] = value

        attend_pairs(place_ref, near_ref, far_ref, x_ref, xt_ref, var_ref, varrow_ref, put, slots, pairs, fold)
    load.wait()
    tokens = x_ref.shape[0]
    feats, model = wp_ref.shape
    x = x_ref[:, :feats]
    tiles = [(at, min(2 * LANES, model - at)) for at in range(0, model, 2 * LANES)]
    sum_buf[...] = jnp.zeros(sum_buf.shape, f32)

    def folded(value):
        total = value[:, :LANES]
        for at in range(LANES, value.shape[1], LANES):
            total = total + value[:, at : at + LANES]
        return total

    for at, size in tiles:
        cols = slice(at, at + size)
        mixed = dot(att_buf[...], wo_buf[:, cols])
        value = dot(x, wp_ref[:, cols]) + mod_ref[0, 2:3, cols] * mixed
        res_buf[:, cols] = value
        sum_buf[...] = sum_buf[...] + folded(value)
    mean = jnp.sum(sum_buf[...], axis=1, keepdims=True) * (1.0 / model)
    sum_buf[...] = jnp.zeros(sum_buf.shape, f32)
    for at, size in tiles:
        cols = slice(at, at + size)
        value = res_buf[:, cols] - mean
        fin_buf[:, cols] = value.astype(bf16)
        sum_buf[...] = sum_buf[...] + folded(value * value)
    spread = jnp.sum(sum_buf[...], axis=1, keepdims=True) * (1.0 / model)
    result = dot(fin_buf[...], wf_ref[...], ((1,), (1,))) * lax.rsqrt(spread + epsilon)
    near = height // 2 + 1
    keep = guide * (near - 2)
    give = (1 - guide) * (near - 2)
    for p in range(height // 2):
        turned = result[p * columns : (p + 1) * columns].T
        for a in range(2):
            r = 2 * p + a
            for b in range(2):
                f = (a * 2 + b) * channels
                piece = turned[f : f + channels]

                @pl.when(jnp.logical_and(r >= keep, r < keep + near))
                def _():
                    mine_ref[r - keep, :, b * columns : (b + 1) * columns] = piece

                @pl.when(jnp.logical_and(r >= give, r < give + near))
                def _():
                    send_ref[r - give, :, b * columns : (b + 1) * columns] = piece.astype(bf16)


def spread_kernel(place_ref, mine_ref, theirs_ref, own_ref, one_ref, two_ref, back_ref):
    offset = place_ref[1]
    guide = place_ref[2]
    near, channels, wide = mine_ref.shape
    columns = wide // 2
    mine = mine_ref[...].reshape(near * channels, wide)
    theirs = theirs_ref[...].reshape(near * channels, wide).astype(f32)
    cond = jnp.where(guide == 0, mine, theirs)
    plain = jnp.where(guide == 0, theirs, mine)
    guided = plain + guidance * (cond - plain)
    high, low = split(guided)
    spot = iota((wide, 2 * columns), 0)
    lane = iota((wide, 2 * columns), 1)
    b = (spot >= columns).astype(jnp.int32)
    col = offset + 2 * (spot - b * columns) + b
    target = jnp.where(lane < columns, lane, jnp.where(lane == columns, -1, lane - 1))
    target = jnp.where(lane > columns + 1, -4 * wide, target)

    def place(distance):
        return jnp.where(col == target + distance * columns, 1.0, 0.0).astype(bf16)

    here = place(0)
    own_ref[...] = dot(high, here) + dot(low, here)
    one_ref[...] = dot(high, place(1)).astype(bf16)
    two_ref[...] = dot(high, place(2)).astype(bf16)
    back_ref[...] = dot(high, place(-1)[:, columns:]).astype(bf16)


def decode_kernel(
    place_ref, own_ref, one_ref, two_ref, back_ref, lat_ref, count_ref, w_ref, den_ref, feat_ref, pad_buf,
    *, width,
):
    guide = place_ref[2]
    place = place_ref[3]
    near, channels, wide = lat_ref.shape
    columns = wide // 2
    fraction = (jnp.full((1, wide), place_ref[4], jnp.int32).astype(f32) + 1.0) / STEPS
    sigma = 3.0 * fraction / (1.0 + 2.0 * fraction)
    total = own_ref[...] + one_ref[...].astype(f32) + two_ref[...].astype(f32)
    back = jnp.concatenate([jnp.zeros(back_ref.shape, f32), back_ref[...].astype(f32)], axis=1)
    velocity = (total + back) / count_ref[:1, :]
    clean = lat_ref[...].reshape(near * channels, wide) - sigma * velocity
    half = near - 1
    first = guide
    lane = iota((near * channels, columns), 1)
    main = clean[:, :columns]
    edges = clean[:, columns:]
    left = jnp.where(place == 0, 0.0, edges[:, 0:1])
    right = jnp.where(place == width - 1, 0.0, edges[:, 1:2])
    before = jnp.where(lane == 0, left, pltpu.roll(main, 1, 1))
    after = jnp.where(lane == columns - 1, right, pltpu.roll(main, columns - 1, 1))
    zero = jnp.zeros((channels, columns), f32)
    for b, value in enumerate((before, main, after)):
        pad_buf[b, 0] = zero
        pad_buf[b, near + 1] = zero
        for i in range(near):
            pad_buf[b, i + 1] = value[i * channels : (i + 1) * channels]
    for r in range(half):
        at = first + r
        den_ref[:, r, :] = pad_buf[1, at + 1]
        stacked = jnp.concatenate(
            [pad_buf[b, at + a] for a in range(3) for b in range(3)], axis=0
        ).astype(bf16)
        summed = dot(stacked, w_ref[...], ((0,), (0,)))
        feat_ref[r] = (summed / (1.0 + jnp.exp(-summed))).astype(bf16)


def shift(x, by):
    peers = lax.axis_size("width")
    return lax.ppermute(x, "width", [(i, (i + by) % peers) for i in range(peers)])


def swap(x, axis):
    return lax.ppermute(x, axis, [(0, 1), (1, 0)])


def gather_major(chunk, fold, direct):
    width = lax.axis_size("width")
    if not direct:
        every = lax.all_gather(chunk, "width")
        every = every.reshape((width // fold, fold) + chunk.shape)
        return lax.dynamic_index_in_dim(every, lax.axis_index("width") % fold, 1, False)
    pieces = [chunk]
    for d in range(1, width // fold):
        route = [(i, (i // fold ^ d) * fold + i % fold) for i in range(width)]
        pieces.append(lax.ppermute(chunk, "width", route))
    return jnp.stack(pieces)


def swap_minor(stack, fold):
    if fold == 1:
        return stack
    width = lax.axis_size("width")
    return lax.ppermute(stack, "width", [(i, i ^ 1) for i in range(width)])


def shards(latent, starts, counts, step_index, cond_mod, w_patch, w_qkv, w_out, w_final, w_dec):
    guide = lax.axis_index("guide")
    place = lax.axis_index("width")
    group = lax.axis_index("groups")
    width = lax.axis_size("width")
    channels, height, columns = latent.shape
    model = w_patch.shape[1]
    feats = w_patch.shape[0]
    features = HEADS * HEAD
    pairs = features // LANES
    halves = 2 if lax.axis_size("groups") == 2 and pairs % 2 == 0 else 1
    local_pairs = pairs // halves
    slots = -(-3 * local_pairs // width)
    if halves == 1:
        group = group * 0
    rows = w_qkv.shape[0]
    fold = 2 if width % 2 == 0 else 1
    depth = width // fold
    direct = depth <= 8 and depth & (depth - 1) == 0
    offset = starts[0] - place * columns
    key = place // fold if direct else 0
    scalars = jnp.stack([group, offset, guide, place, step_index[0], key]).astype(jnp.int32)

    pack = jnp.concatenate(
        [latent, jnp.broadcast_to(counts.astype(f32)[None, None, :], (1, height, columns))], axis=0
    )
    right = shift(pack, -1)
    further = shift(latent.astype(bf16), -2)
    left = shift(pack, 1)

    (parts,) = call(
        functools.partial(
            partial_kernel, width=width, slots=slots, local_pairs=local_pairs, features=features
        ),
        [((width, ROWS, slots * LANES), bf16)],
        scratch=[
            pltpu.VMEM((3, rows, local_pairs * LANES), bf16),
            pltpu.SemaphoreType.DMA((3,)),
        ],
        anys=(3,), smem=(0,), count=4,
    )(scalars, cond_mod, w_patch, w_qkv)
    parts = lax.all_to_all(parts, "width", 0, 0, tiled=True)
    (chunk,) = call(
        functools.partial(sum_kernel, width=width), [((ROWS, slots * LANES), bf16)], count=1
    )(parts)
    near = height // 2 + 1
    tokens = height // 2 * columns
    x, xt, var, varrow, lat, count = call(
        window_kernel,
        [
            ((tokens, LANES), bf16), ((ROWS, tokens), bf16), ((tokens, LANES), f32),
            ((8, tokens), f32), ((near, channels, 2 * columns), f32), ((height, 2 * columns), f32),
        ],
        scratch=[
            pltpu.VMEM((height * channels, 3 * columns), bf16),
            pltpu.VMEM((feats, tokens), f32),
            pltpu.VMEM((tokens, model), f32),
        ],
        smem=(0,), count=6, flops=5e9,
    )(scalars, pack, right, left, further, w_patch)
    stack = gather_major(chunk, fold, direct)
    side = swap_minor(stack, fold)
    if halves == 2:
        stack_x, side_x = swap(stack, "groups"), swap(side, "groups")
    else:
        stack_x, side_x = stack, side
    (att,) = call(
        functools.partial(first_kernel, slots=slots, pairs=local_pairs, fold=fold),
        [((tokens, local_pairs * LANES), bf16)],
        smem=(0,), count=7, flops=6e9,
    )(scalars, stack, side, x, xt, var, varrow)
    mine_v, send_v = call(
        functools.partial(
            second_kernel, slots=slots, pairs=local_pairs, channels=channels, height=height,
            columns=columns, halves=halves, fold=fold,
        ),
        [((near, channels, 2 * columns), f32), ((near, channels, 2 * columns), bf16)],
        scratch=[
            pltpu.VMEM((tokens, features), bf16),
            pltpu.VMEM(w_out.shape, bf16),
            pltpu.VMEM((tokens, model), f32),
            pltpu.VMEM((tokens, model), bf16),
            pltpu.VMEM((tokens, LANES), f32),
            pltpu.SemaphoreType.DMA((1,)),
        ],
        anys=(11,), smem=(0,), count=12, flops=12e9,
    )(scalars, stack_x, side_x, x, xt, var, varrow, att, w_patch, cond_mod, w_final.T, w_out)
    theirs = swap(send_v, "guide")
    flat = near * channels
    own, one, two, back = call(
        spread_kernel,
        [
            ((flat, 2 * columns), f32), ((flat, 2 * columns), bf16),
            ((flat, 2 * columns), bf16), ((flat, columns), bf16),
        ],
        smem=(0,), count=3,
    )(scalars, mine_v, theirs)
    one = shift(one, 1)
    two = shift(two, 2)
    back = shift(back, -1)
    return call(
        functools.partial(decode_kernel, width=width),
        [((channels, height // 2, columns), f32), ((height // 2, columns, w_dec.shape[1]), bf16)],
        scratch=[pltpu.VMEM((3, near + 2, channels, columns), f32)],
        smem=(0,), count=8,
    )(scalars, own, one, two, back, lat, count, w_dec)


def solution(mesh):
    return jax.shard_map(
        shards,
        mesh=mesh,
        in_specs=(
            P(None, None, ("groups", "width")),
            P(("groups", "width")),
            P(("groups", "width")),
            P("groups"),
            P("guide", None, None),
            P(),
            P("width", None),
            P(),
            P(),
            P(),
        ),
        out_specs=(P(None, "guide", ("groups", "width")), P("guide", ("groups", "width"), None)),
        check_vma=False,
    )
```

```python
import functools

import jax
import jax.numpy as jnp
from jax import lax
from jax.experimental import pallas as pl
from jax.experimental.pallas import tpu as pltpu
from jax.sharding import PartitionSpec as P

HEADS = 20
HEAD = 64
STEPS = 28
LANES = 128
ROWS = 72

guidance = 4.0
epsilon = 1e-06

bf16 = jnp.bfloat16
f32 = jnp.float32
PARTS = (0, 2, 1)
LOG2E = 1.4426950408889634


def dot(a, b, dims=((1,), (0,))):
    return lax.dot_general(a, b, (dims, ((), ())), preferred_element_type=f32)


def call(body, outs, scratch=(), anys=(), smem=(), count=0, limit=16, flops=0):
    def spec(i):
        if i in anys:
            return pl.BlockSpec(memory_space=pltpu.HBM)
        if i in smem:
            return pl.BlockSpec(memory_space=pltpu.SMEM)
        return pl.BlockSpec(memory_space=pltpu.VMEM)

    return pl.pallas_call(
        body,
        out_shape=tuple(jax.ShapeDtypeStruct(s, t) for s, t in outs),
        in_specs=[spec(i) for i in range(count)],
        out_specs=tuple(pl.BlockSpec(memory_space=pltpu.VMEM) for _ in outs),
        scratch_shapes=list(scratch),
        compiler_params=pltpu.CompilerParams(vmem_limit_bytes=limit << 20),
        cost_estimate=pl.CostEstimate(flops=int(flops), bytes_accessed=1 << 20, transcendentals=0),
    )


def iota(shape, dim):
    return lax.broadcasted_iota(jnp.int32, shape, dim)


def split(values):
    high = values.astype(bf16)
    return high, (values - high.astype(f32)).astype(bf16)


def partial_kernel(
    place_ref, mod_ref, wp_ref, w_ref, out_ref, w_buf, sems, *, width, slots, local_pairs, features
):
    group = place_ref[0]
    span = local_pairs * LANES
    copies = []
    for part in range(3):
        start = pl.multiple_of(part * features + group * span, LANES)
        copies.append(
            pltpu.make_async_copy(w_ref.at[:, pl.ds(start, span)], w_buf.at[part], sems.at[part])
        )
    for one in copies:
        one.start()
    feats, model = wp_ref.shape
    rows = w_buf.shape[1]
    window = min(model, -(-(rows + LANES - 1) // LANES) * LANES)
    begin = place_ref[3] * rows
    low = jnp.minimum(begin // LANES * LANES, model - window)
    cols = pl.ds(pl.multiple_of(low, LANES), window)
    mean = jnp.sum(wp_ref[...].astype(f32), axis=1, keepdims=True) * (1.0 / model)
    centered = wp_ref[:, cols].astype(f32) - mean
    scaled = centered * (1.0 + mod_ref[1, :, cols])
    down = iota((ROWS - feats, window), 0)
    tail = jnp.where(down < 2, jnp.broadcast_to(mod_ref[0, :, cols], down.shape), 0.0)
    stacked = jnp.concatenate([scaled, tail], axis=0)
    stacked = pltpu.roll(stacked, (window - (begin - low)) % window, 1)
    a = jnp.concatenate(split(stacked), axis=0)[:, :rows]
    for one in copies:
        one.wait()
    for owner in range(width):
        for slot in range(slots):
            tile = owner * slots + slot
            if tile < 3 * local_pairs:
                pair, sub = divmod(tile, 3)
                both = dot(a, w_buf[PARTS[sub], :, pair * LANES : (pair + 1) * LANES])
                value = (both[:ROWS] + both[ROWS:]).astype(bf16)
            else:
                value = jnp.zeros((ROWS, LANES), bf16)
            out_ref[owner, :, slot * LANES : (slot + 1) * LANES] = value


def sum_kernel(parts_ref, out_ref, *, width):
    total = parts_ref[0].astype(f32)
    for i in range(1, width):
        total = total + parts_ref[i].astype(f32)
    out_ref[...] = total.astype(bf16)


def window_kernel(
    place_ref, own_ref, right_ref, left_ref, further_ref, w_ref,
    x_ref, xt_ref, var_ref, varrow_ref, lat_ref, count_ref,
    rows_buf, xt_buf, hid_buf,
):
    channels, height, columns = own_ref.shape[0] - 1, own_ref.shape[1], own_ref.shape[2]
    offset = place_ref[1]
    guide = place_ref[2]
    near = height // 2 + 1
    lane = iota((channels, LANES), 1)
    for r in range(height):
        at = slice(r * channels, (r + 1) * channels)
        rows_buf[at, :columns] = own_ref[:channels, r, :].astype(bf16)
        rows_buf[at, columns : 2 * columns] = right_ref[:channels, r, :].astype(bf16)
        rows_buf[at, 2 * columns :] = further_ref[:, r, :]
    col = iota((3 * columns, 2 * columns), 0)
    spot = iota((3 * columns, 2 * columns), 1)
    b = (spot >= columns).astype(jnp.int32)
    pick = jnp.where(col == offset + 2 * (spot - b * columns) + b, 1.0, 0.0).astype(bf16)
    placed = dot(rows_buf[...], pick).astype(bf16)
    tokens = height // 2 * columns
    for p in range(height // 2):
        for a in range(2):
            for b in range(2):
                f = (a * 2 + b) * channels
                xt_buf[f : f + channels, p * columns : (p + 1) * columns] = placed[
                    (2 * p + a) * channels : (2 * p + a + 1) * channels, b * columns : (b + 1) * columns
                ].astype(f32)
    feats = 4 * channels
    xt = xt_buf[:feats, :]
    xpad = jnp.concatenate([xt, jnp.zeros((LANES - feats, tokens), f32)], axis=0)
    xrow = xpad.T
    model = w_ref.shape[1]
    block = 64
    x_bf = xrow[:, :feats].astype(bf16)
    hid_buf[...] = dot(x_bf, w_ref[...])

    def stats(i, carry):
        at = pl.ds(pl.multiple_of(i * block, block), block)
        h = hid_buf[at, :]
        mean = jnp.sum(h, axis=1, keepdims=True) * (1.0 / model)
        c = h - mean
        v = jnp.sum(c * c, axis=1, keepdims=True) * (1.0 / model)
        var_ref[at, :] = jnp.broadcast_to(v, (block, LANES))
        return carry

    lax.fori_loop(0, tokens // block, stats, 0)
    var = var_ref[...]
    std_hi, std_lo = split(jnp.sqrt(var + epsilon))
    spots = iota((tokens, LANES), 1)
    x_ref[...] = jnp.where(
        spots == feats, std_hi.astype(f32), jnp.where(spots == feats + 1, std_lo.astype(f32), xrow)
    ).astype(bf16)
    var_t = var.T[:8]
    varrow_ref[...] = var_t
    hi_t, lo_t = split(jnp.sqrt(var_t + epsilon))
    down = iota((8, tokens), 0)
    tail = jnp.where(down == 0, hi_t.astype(f32), jnp.where(down == 1, lo_t.astype(f32), 0.0))
    xt_ref[...] = jnp.concatenate([xt, tail], axis=0).astype(bf16)
    first = guide * (near - 2)
    for i in range(near):
        r = pl.ds(first + i, 1)
        lat_ref[i, :, :columns] = own_ref[:channels, r, :].reshape(channels, columns)
        before = pltpu.roll(left_ref[:channels, r, :].reshape(channels, columns), 1, 1)
        after = pltpu.roll(right_ref[:channels, r, :].reshape(channels, columns), 1, 1)
        lat_ref[i, :, columns:] = jnp.where(lane == 0, before, jnp.where(lane == 1, after, 0.0))
    lane8 = iota((height, LANES), 1)
    count_ref[:, :columns] = own_ref[channels]
    before = pltpu.roll(left_ref[channels], 1, 1)
    after = pltpu.roll(right_ref[channels], 1, 1)
    count_ref[:, columns:] = jnp.where(lane8 == 0, before, jnp.where(lane8 == 1, after, 1.0))


def attend_pairs(place_ref, near_ref, far_ref, x_ref, xt_ref, var_ref, varrow_ref, put, slots, pairs, fold):
    tokens = x_ref.shape[0]
    key = place_ref[5]
    side = place_ref[3] % fold
    x = x_ref[:, :ROWS]
    xt = xt_ref[...]
    var = var_ref[...]
    eps_col = epsilon * (var + epsilon)
    rstd = lax.rsqrt(var + epsilon)
    eps_row = epsilon * (varrow_ref[:1, :] + epsilon)
    low = iota((tokens, LANES), 1) < HEAD
    scale = LOG2E * HEAD**-0.5

    def tile(t):
        owner, slot = divmod(t, slots)
        z, y = divmod(owner, fold)
        at = (z ^ key, slice(None), slice(slot * LANES, (slot + 1) * LANES))
        return jnp.where(side == y, near_ref[at], far_ref[at])

    for pair in range(pairs):
        mq, mv, mk = (tile(3 * pair + sub) for sub in range(3))
        both = dot(x, jnp.concatenate([mq, mv], axis=1))
        uq = both[:, :LANES]
        uv = both[:, LANES:] * rstd
        uk = dot(mk, xt, ((0,), (0,)))
        sq = uq * uq
        sum_low = jnp.sum(jnp.where(low, sq, 0.0), axis=1, keepdims=True)
        sum_high = jnp.sum(jnp.where(low, 0.0, sq), axis=1, keepdims=True)
        q = uq * lax.rsqrt(jnp.where(low, sum_low, sum_high) * (1.0 / HEAD) + eps_col)
        keys = []
        for half in range(2):
            k = uk[half * HEAD : (half + 1) * HEAD]
            mean = jnp.sum(k * k, axis=0, keepdims=True) * (1.0 / HEAD)
            keys.append((k * lax.rsqrt(mean + eps_row)).astype(bf16))
        kt = jnp.concatenate(keys, axis=0)
        outs = []
        for half in range(2):
            mine = low if half == 0 else jnp.logical_not(low)
            qh = jnp.where(mine, q, 0.0).astype(bf16)
            vh = jnp.where(mine, uv, 1.0).astype(bf16)
            weights = jnp.exp2(dot(qh, kt) * scale).astype(bf16)
            outs.append(dot(weights, vh))
        top = jnp.where(low, outs[0], outs[1])
        sums = pltpu.roll(jnp.where(low, outs[1], outs[0]), HEAD, 1)
        put(pair, (top / sums).astype(bf16))


def first_kernel(
    place_ref, near_ref, far_ref, x_ref, xt_ref, var_ref, varrow_ref, att_ref, *, slots, pairs, fold
):
    def put(pair, value):
        att_ref[:, pair * LANES : (pair + 1) * LANES] = value

    attend_pairs(place_ref, near_ref, far_ref, x_ref, xt_ref, var_ref, varrow_ref, put, slots, pairs, fold)


def second_kernel(
    place_ref, near_ref, far_ref, x_ref, xt_ref, var_ref, varrow_ref, att_ref, wp_ref, mod_ref, wf_ref, wo_ref,
    mine_ref, send_ref,
    att_buf, res_buf, fin_buf, sum_buf,
    *, slots, pairs, channels, height, columns, halves, fold,
):
    group = place_ref[0]
    guide = place_ref[2]
    span = pairs * LANES
    first = pl.multiple_of(group * span, LANES) if halves == 2 else 0
    att_buf[:, pl.ds(first, span)] = att_ref[...]
    if halves == 2:
        other = (1 - group) * span

        def put(pair, value):
            at = pl.multiple_of(other + pair * LANES, LANES)
            att_buf[:, pl.ds(at, LANES)] = value

        attend_pairs(place_ref, near_ref, far_ref, x_ref, xt_ref, var_ref, varrow_ref, put, slots, pairs, fold)
    tokens = x_ref.shape[0]
    feats, model = wp_ref.shape
    x = x_ref[:, :feats]
    tiles = [(at, min(2 * LANES, model - at)) for at in range(0, model, 2 * LANES)]
    sum_buf[...] = jnp.zeros(sum_buf.shape, f32)

    def folded(value):
        total = value[:, :LANES]
        for at in range(LANES, value.shape[1], LANES):
            total = total + value[:, at : at + LANES]
        return total

    for at, size in tiles:
        cols = slice(at, at + size)
        mixed = dot(att_buf[...], wo_ref[:, cols])
        value = dot(x, wp_ref[:, cols]) + mod_ref[2, :, cols] * mixed
        res_buf[:, cols] = value
        sum_buf[...] = sum_buf[...] + folded(value)
    mean = jnp.sum(sum_buf[...], axis=1, keepdims=True) * (1.0 / model)
    sum_buf[...] = jnp.zeros(sum_buf.shape, f32)
    for at, size in tiles:
        cols = slice(at, at + size)
        value = res_buf[:, cols] - mean
        fin_buf[:, cols] = value.astype(bf16)
        sum_buf[...] = sum_buf[...] + folded(value * value)
    spread = jnp.sum(sum_buf[...], axis=1, keepdims=True) * (1.0 / model)
    result = dot(fin_buf[...], wf_ref[...], ((1,), (1,))) * lax.rsqrt(spread + epsilon)
    near = height // 2 + 1
    keep = guide * (near - 2)
    give = (1 - guide) * (near - 2)
    for p in range(height // 2):
        turned = result[p * columns : (p + 1) * columns].T
        for a in range(2):
            r = 2 * p + a
            for b in range(2):
                f = (a * 2 + b) * channels
                piece = turned[f : f + channels]

                @pl.when(jnp.logical_and(r >= keep, r < keep + near))
                def _():
                    mine_ref[r - keep, :, b * columns : (b + 1) * columns] = piece

                @pl.when(jnp.logical_and(r >= give, r < give + near))
                def _():
                    send_ref[r - give, :, b * columns : (b + 1) * columns] = piece.astype(bf16)


def spread_kernel(place_ref, mine_ref, theirs_ref, own_ref, one_ref, two_ref, back_ref):
    offset = place_ref[1]
    guide = place_ref[2]
    near, channels, wide = mine_ref.shape
    columns = wide // 2
    mine = mine_ref[...].reshape(near * channels, wide)
    theirs = theirs_ref[...].reshape(near * channels, wide).astype(f32)
    cond = jnp.where(guide == 0, mine, theirs)
    plain = jnp.where(guide == 0, theirs, mine)
    guided = plain + guidance * (cond - plain)
    high, low = split(guided)
    spot = iota((wide, 2 * columns), 0)
    lane = iota((wide, 2 * columns), 1)
    b = (spot >= columns).astype(jnp.int32)
    col = offset + 2 * (spot - b * columns) + b
    target = jnp.where(lane < columns, lane, jnp.where(lane == columns, -1, lane - 1))
    target = jnp.where(lane > columns + 1, -4 * wide, target)

    def place(distance):
        return jnp.where(col == target + distance * columns, 1.0, 0.0).astype(bf16)

    here = place(0)
    own_ref[...] = dot(high, here) + dot(low, here)
    one_ref[...] = dot(high, place(1)).astype(bf16)
    two_ref[...] = dot(high, place(2)).astype(bf16)
    back_ref[...] = dot(high, place(-1)[:, columns:]).astype(bf16)


def decode_kernel(
    place_ref, own_ref, one_ref, two_ref, back_ref, lat_ref, count_ref, w_ref, den_ref, feat_ref, pad_buf,
    *, width,
):
    guide = place_ref[2]
    place = place_ref[3]
    near, channels, wide = lat_ref.shape
    columns = wide // 2
    fraction = (jnp.full((1, wide), place_ref[4], jnp.int32).astype(f32) + 1.0) / STEPS
    sigma = 3.0 * fraction / (1.0 + 2.0 * fraction)
    total = own_ref[...] + one_ref[...].astype(f32) + two_ref[...].astype(f32)
    back = jnp.concatenate([jnp.zeros(back_ref.shape, f32), back_ref[...].astype(f32)], axis=1)
    velocity = (total + back) / count_ref[:1, :]
    clean = lat_ref[...].reshape(near * channels, wide) - sigma * velocity
    half = near - 1
    first = guide
    lane = iota((near * channels, columns), 1)
    main = clean[:, :columns]
    edges = clean[:, columns:]
    left = jnp.where(place == 0, 0.0, edges[:, 0:1])
    right = jnp.where(place == width - 1, 0.0, edges[:, 1:2])
    before = jnp.where(lane == 0, left, pltpu.roll(main, 1, 1))
    after = jnp.where(lane == columns - 1, right, pltpu.roll(main, columns - 1, 1))
    zero = jnp.zeros((channels, columns), f32)
    for b, value in enumerate((before, main, after)):
        pad_buf[b, 0] = zero
        pad_buf[b, near + 1] = zero
        for i in range(near):
            pad_buf[b, i + 1] = value[i * channels : (i + 1) * channels]
    for r in range(half):
        at = first + r
        den_ref[:, r, :] = pad_buf[1, at + 1]
        stacked = jnp.concatenate(
            [pad_buf[b, at + a] for a in range(3) for b in range(3)], axis=0
        ).astype(bf16)
        summed = dot(stacked, w_ref[...], ((0,), (0,)))
        feat_ref[r] = (summed / (1.0 + jnp.exp(-summed))).astype(bf16)


def shift(x, by):
    peers = lax.axis_size("width")
    return lax.ppermute(x, "width", [(i, (i + by) % peers) for i in range(peers)])


def swap(x, axis):
    return lax.ppermute(x, axis, [(0, 1), (1, 0)])


def gather_major(chunk, fold, direct):
    width = lax.axis_size("width")
    if not direct:
        every = lax.all_gather(chunk, "width")
        every = every.reshape((width // fold, fold) + chunk.shape)
        return lax.dynamic_index_in_dim(every, lax.axis_index("width") % fold, 1, False)
    pieces = [chunk]
    for d in range(1, width // fold):
        route = [(i, (i // fold ^ d) * fold + i % fold) for i in range(width)]
        pieces.append(lax.ppermute(chunk, "width", route))
    return jnp.stack(pieces)


def swap_minor(stack, fold):
    if fold == 1:
        return stack
    width = lax.axis_size("width")
    return lax.ppermute(stack, "width", [(i, i ^ 1) for i in range(width)])


def shards(latent, starts, counts, step_index, cond_mod, w_patch, w_qkv, w_out, w_final, w_dec):
    guide = lax.axis_index("guide")
    place = lax.axis_index("width")
    group = lax.axis_index("groups")
    width = lax.axis_size("width")
    channels, height, columns = latent.shape
    model = w_patch.shape[1]
    feats = w_patch.shape[0]
    features = HEADS * HEAD
    pairs = features // LANES
    halves = 2 if lax.axis_size("groups") == 2 and pairs % 2 == 0 else 1
    local_pairs = pairs // halves
    slots = -(-3 * local_pairs // width)
    if halves == 1:
        group = group * 0
    rows = w_qkv.shape[0]
    fold = 2 if width % 2 == 0 else 1
    depth = width // fold
    direct = depth <= 8 and depth & (depth - 1) == 0
    changes = jnp.swapaxes(cond_mod, 0, 1)
    offset = starts[0] - place * columns
    key = place // fold if direct else 0
    scalars = jnp.stack([group, offset, guide, place, step_index[0], key]).astype(jnp.int32)

    (parts,) = call(
        functools.partial(
            partial_kernel, width=width, slots=slots, local_pairs=local_pairs, features=features
        ),
        [((width, ROWS, slots * LANES), bf16)],
        scratch=[
            pltpu.VMEM((3, rows, local_pairs * LANES), bf16),
            pltpu.SemaphoreType.DMA((3,)),
        ],
        anys=(3,), smem=(0,), count=4, limit=8,
    )(scalars, changes, w_patch, pltpu.with_memory_space_constraint(w_qkv, pltpu.HBM))
    latent_now, counts_now, parts = lax.optimization_barrier((latent, counts, parts))
    pack = jnp.concatenate(
        [latent_now, jnp.broadcast_to(counts_now.astype(f32)[None, None, :], (1, height, columns))], axis=0
    )
    right = shift(pack, -1)
    further = shift(latent_now.astype(bf16), -2)
    left = shift(pack, 1)

    parts = lax.all_to_all(parts, "width", 0, 0, tiled=True)
    near = height // 2 + 1
    tokens = height // 2 * columns
    x, xt, var, varrow, lat, count = call(
        window_kernel,
        [
            ((tokens, LANES), bf16), ((ROWS, tokens), bf16), ((tokens, LANES), f32),
            ((8, tokens), f32), ((near, channels, 2 * columns), f32), ((height, 2 * columns), f32),
        ],
        scratch=[
            pltpu.VMEM((height * channels, 3 * columns), bf16),
            pltpu.VMEM((feats, tokens), f32),
            pltpu.VMEM((tokens, model), f32),
        ],
        smem=(0,), count=6, flops=5e9,
    )(scalars, pack, right, left, further, w_patch)
    parts, x = lax.optimization_barrier((parts, x))
    (chunk,) = call(
        functools.partial(sum_kernel, width=width), [((ROWS, slots * LANES), bf16)], count=1, limit=4
    )(parts)
    stack = gather_major(chunk, fold, direct)
    side = swap_minor(stack, fold)
    if halves == 2:
        stack_x, side_x = swap(stack, "groups"), swap(side, "groups")
    else:
        stack_x, side_x = stack, side
    (att,) = call(
        functools.partial(first_kernel, slots=slots, pairs=local_pairs, fold=fold),
        [((tokens, local_pairs * LANES), bf16)],
        smem=(0,), count=7, flops=6e9,
    )(scalars, stack, side, x, xt, var, varrow)
    mine_v, send_v = call(
        functools.partial(
            second_kernel, slots=slots, pairs=local_pairs, channels=channels, height=height,
            columns=columns, halves=halves, fold=fold,
        ),
        [((near, channels, 2 * columns), f32), ((near, channels, 2 * columns), bf16)],
        scratch=[
            pltpu.VMEM((tokens, features), bf16),
            pltpu.VMEM((tokens, model), f32),
            pltpu.VMEM((tokens, model), bf16),
            pltpu.VMEM((tokens, LANES), f32),
        ],
        smem=(0,), count=12, flops=12e9, limit=22,
    )(scalars, stack_x, side_x, x, xt, var, varrow, att, w_patch, changes, w_final.T, w_out)
    theirs = swap(send_v, "guide")
    flat = near * channels
    own, one, two, back = call(
        spread_kernel,
        [
            ((flat, 2 * columns), f32), ((flat, 2 * columns), bf16),
            ((flat, 2 * columns), bf16), ((flat, columns), bf16),
        ],
        smem=(0,), count=3,
    )(scalars, mine_v, theirs)
    one = shift(one, 1)
    two = shift(two, 2)
    back = shift(back, -1)
    return call(
        functools.partial(decode_kernel, width=width),
        [((channels, height // 2, columns), f32), ((height // 2, columns, w_dec.shape[1]), bf16)],
        scratch=[pltpu.VMEM((3, near + 2, channels, columns), f32)],
        smem=(0,), count=8,
    )(scalars, own, one, two, back, lat, count, w_dec)


def solution(mesh):
    return jax.shard_map(
        shards,
        mesh=mesh,
        in_specs=(
            P(None, None, ("groups", "width")),
            P(("groups", "width")),
            P(("groups", "width")),
            P("groups"),
            P("guide", None, None),
            P(),
            P("width", None),
            P(),
            P(),
            P(),
        ),
        out_specs=(P(None, "guide", ("groups", "width")), P("guide", ("groups", "width"), None)),
        check_vma=False,
    )
```

```python
import functools

import jax
import jax.numpy as jnp
from jax import lax
from jax.experimental import pallas as pl
from jax.experimental.pallas import tpu as pltpu
from jax.sharding import PartitionSpec as P

HEADS = 20
HEAD = 64
STEPS = 28
LANES = 128
ROWS = 72

guidance = 4.0
epsilon = 1e-06

bf16 = jnp.bfloat16
f32 = jnp.float32
PARTS = (0, 2, 1)
LOG2E = 1.4426950408889634


def dot(a, b, dims=((1,), (0,))):
    return lax.dot_general(a, b, (dims, ((), ())), preferred_element_type=f32)


def call(body, outs, scratch=(), anys=(), smem=(), count=0, limit=16, flops=0):
    def spec(i):
        if i in anys:
            return pl.BlockSpec(memory_space=pltpu.HBM)
        if i in smem:
            return pl.BlockSpec(memory_space=pltpu.SMEM)
        return pl.BlockSpec(memory_space=pltpu.VMEM)

    return pl.pallas_call(
        body,
        out_shape=tuple(jax.ShapeDtypeStruct(s, t) for s, t in outs),
        in_specs=[spec(i) for i in range(count)],
        out_specs=tuple(pl.BlockSpec(memory_space=pltpu.VMEM) for _ in outs),
        scratch_shapes=list(scratch),
        compiler_params=pltpu.CompilerParams(vmem_limit_bytes=limit << 20),
        cost_estimate=pl.CostEstimate(flops=int(flops), bytes_accessed=1 << 20, transcendentals=0),
    )


def iota(shape, dim):
    return lax.broadcasted_iota(jnp.int32, shape, dim)


def split(values):
    high = values.astype(bf16)
    return high, (values - high.astype(f32)).astype(bf16)


def partial_kernel(
    place_ref, mod_ref, wp_ref, w_ref, *refs, width, slots, local_pairs, features, fold, direct
):
    *out_refs, w_buf, mod_buf, wp_buf, sems = refs
    group = place_ref[0]
    span = local_pairs * LANES
    loads = [
        pltpu.make_async_copy(wp_ref, wp_buf, sems.at[0]),
        pltpu.make_async_copy(mod_ref, mod_buf, sems.at[1]),
    ]
    for part in range(3):
        start = pl.multiple_of(part * features + group * span, LANES)
        loads.append(
            pltpu.make_async_copy(w_ref.at[:, pl.ds(start, span)], w_buf.at[part], sems.at[2 + part])
        )
    for one in loads:
        one.start()
    feats, model = wp_ref.shape
    rows = w_buf.shape[1]
    window = min(model, -(-(rows + LANES - 1) // LANES) * LANES)
    begin = place_ref[3] * rows
    low = jnp.minimum(begin // LANES * LANES, model - window)
    cols = pl.ds(pl.multiple_of(low, LANES), window)
    loads[0].wait()
    loads[1].wait()
    mean = jnp.sum(wp_buf[...].astype(f32), axis=1, keepdims=True) * (1.0 / model)
    centered = wp_buf[:, cols].astype(f32) - mean
    scaled = centered * (1.0 + mod_buf[1, :, cols])
    down = iota((ROWS - feats, window), 0)
    tail = jnp.where(down < 2, jnp.broadcast_to(mod_buf[0, :, cols], down.shape), 0.0)
    stacked = jnp.concatenate([scaled, tail], axis=0)
    stacked = pltpu.roll(stacked, (window - (begin - low)) % window, 1)
    a = jnp.concatenate(split(stacked), axis=0)[:, :rows]
    for one in loads[2:]:
        one.wait()
    side = place_ref[3] % fold
    for owner in range(width):
        pieces = []
        for slot in range(slots):
            tile = owner * slots + slot
            if tile < 3 * local_pairs:
                pair, sub = divmod(tile, 3)
                both = dot(a, w_buf[PARTS[sub], :, pair * LANES : (pair + 1) * LANES])
                pieces.append(both[:ROWS] + both[ROWS:])
            else:
                pieces.append(jnp.zeros((ROWS, LANES), f32))
        value = jnp.concatenate(pieces, axis=1)
        if not direct:
            out_refs[0][owner] = value.astype(bf16)
            continue
        z, y = divmod(owner, fold)

        @pl.when(side == y)
        def _():
            out_refs[0][z] = value

        @pl.when(side != y)
        def _():
            out_refs[1][z] = value.astype(bf16)


def sum_kernel(parts_ref, out_ref, *, width):
    total = parts_ref[0].astype(f32)
    for i in range(1, width):
        total = total + parts_ref[i].astype(f32)
    out_ref[...] = total.astype(bf16)


def first_sum_kernel(place_ref, keep_ref, came_ref, own_ref, *send_refs):
    key = place_ref[5]
    own_ref[...] = keep_ref[key] + came_ref[key].astype(f32)
    for d, ref in enumerate(send_refs):
        at = key ^ (d + 1)
        ref[...] = (keep_ref[at] + came_ref[at].astype(f32)).astype(bf16)


def last_sum_kernel(*refs):
    *parts, out_ref = refs
    total = parts[0][...]
    for ref in parts[1:]:
        total = total + ref[...].astype(f32)
    out_ref[...] = total.astype(bf16)


def window_kernel(
    place_ref, own_ref, right_ref, further_ref, wp_ref,
    x_ref, xt_ref, var_ref, varrow_ref,
    rows_buf, xt_buf, hid_buf, w_ref, sem,
):
    load = pltpu.make_async_copy(wp_ref, w_ref, sem.at[0])
    load.start()
    channels, height, columns = own_ref.shape
    offset = place_ref[1]
    for r in range(height):
        at = slice(r * channels, (r + 1) * channels)
        rows_buf[at, :columns] = own_ref[:, r, :].astype(bf16)
        rows_buf[at, columns : 2 * columns] = right_ref[:, r, :].astype(bf16)
        rows_buf[at, 2 * columns :] = further_ref[:, r, :].astype(bf16)
    col = iota((3 * columns, 2 * columns), 0)
    spot = iota((3 * columns, 2 * columns), 1)
    b = (spot >= columns).astype(jnp.int32)
    pick = jnp.where(col == offset + 2 * (spot - b * columns) + b, 1.0, 0.0).astype(bf16)
    placed = dot(rows_buf[...], pick).astype(bf16)
    tokens = height // 2 * columns
    for p in range(height // 2):
        for a in range(2):
            for b in range(2):
                f = (a * 2 + b) * channels
                xt_buf[f : f + channels, p * columns : (p + 1) * columns] = placed[
                    (2 * p + a) * channels : (2 * p + a + 1) * channels, b * columns : (b + 1) * columns
                ].astype(f32)
    feats = 4 * channels
    xt = xt_buf[:feats, :]
    xpad = jnp.concatenate([xt, jnp.zeros((LANES - feats, tokens), f32)], axis=0)
    xrow = xpad.T
    model = w_ref.shape[1]
    block = 64
    x_bf = xrow[:, :feats].astype(bf16)
    load.wait()
    hid_buf[...] = dot(x_bf, w_ref[...])

    def stats(i, carry):
        at = pl.ds(pl.multiple_of(i * block, block), block)
        h = hid_buf[at, :]
        mean = jnp.sum(h, axis=1, keepdims=True) * (1.0 / model)
        c = h - mean
        v = jnp.sum(c * c, axis=1, keepdims=True) * (1.0 / model)
        var_ref[at, :] = jnp.broadcast_to(v, (block, LANES))
        return carry

    lax.fori_loop(0, tokens // block, stats, 0)
    var = var_ref[...]
    std_hi, std_lo = split(jnp.sqrt(var + epsilon))
    spots = iota((tokens, LANES), 1)
    x_ref[...] = jnp.where(
        spots == feats, std_hi.astype(f32), jnp.where(spots == feats + 1, std_lo.astype(f32), xrow)
    ).astype(bf16)
    var_t = var.T[:8]
    varrow_ref[...] = var_t
    hi_t, lo_t = split(jnp.sqrt(var_t + epsilon))
    down = iota((8, tokens), 0)
    tail = jnp.where(down == 0, hi_t.astype(f32), jnp.where(down == 1, lo_t.astype(f32), 0.0))
    xt_ref[...] = jnp.concatenate([xt, tail], axis=0).astype(bf16)


def attend_pairs(place_ref, near_ref, far_ref, x_ref, xt_ref, var_ref, varrow_ref, put, slots, pairs, fold):
    tokens = x_ref.shape[0]
    key = place_ref[5]
    side = place_ref[3] % fold
    x = x_ref[:, :ROWS]
    xt = xt_ref[...]
    var = var_ref[...]
    eps_col = epsilon * (var + epsilon)
    rstd = lax.rsqrt(var + epsilon)
    eps_row = epsilon * (varrow_ref[:1, :] + epsilon)
    low = iota((tokens, LANES), 1) < HEAD
    scale = LOG2E * HEAD**-0.5

    def tile(t):
        owner, slot = divmod(t, slots)
        z, y = divmod(owner, fold)
        at = (z ^ key, slice(None), slice(slot * LANES, (slot + 1) * LANES))
        return jnp.where(side == y, near_ref[at], far_ref[at])

    for pair in range(pairs):
        mq, mv, mk = (tile(3 * pair + sub) for sub in range(3))
        both = dot(x, jnp.concatenate([mq, mv], axis=1))
        uq = both[:, :LANES]
        uv = both[:, LANES:] * rstd
        uk = dot(mk, xt, ((0,), (0,)))
        sq = uq * uq
        sum_low = jnp.sum(jnp.where(low, sq, 0.0), axis=1, keepdims=True)
        sum_high = jnp.sum(jnp.where(low, 0.0, sq), axis=1, keepdims=True)
        q = uq * lax.rsqrt(jnp.where(low, sum_low, sum_high) * (1.0 / HEAD) + eps_col)
        keys = []
        for half in range(2):
            k = uk[half * HEAD : (half + 1) * HEAD]
            mean = jnp.sum(k * k, axis=0, keepdims=True) * (1.0 / HEAD)
            keys.append((k * lax.rsqrt(mean + eps_row)).astype(bf16))
        kt = jnp.concatenate(keys, axis=0)
        outs = []
        for half in range(2):
            mine = low if half == 0 else jnp.logical_not(low)
            qh = jnp.where(mine, q, 0.0).astype(bf16)
            vh = jnp.where(mine, uv, 1.0).astype(bf16)
            weights = jnp.exp2(dot(qh, kt) * scale).astype(bf16)
            outs.append(dot(weights, vh))
        top = jnp.where(low, outs[0], outs[1])
        sums = pltpu.roll(jnp.where(low, outs[1], outs[0]), HEAD, 1)
        put(pair, (top / sums).astype(bf16))


def first_kernel(
    place_ref, near_ref, far_ref, x_ref, xt_ref, var_ref, varrow_ref, att_ref, *, slots, pairs, fold
):
    def put(pair, value):
        att_ref[:, pair * LANES : (pair + 1) * LANES] = value

    attend_pairs(place_ref, near_ref, far_ref, x_ref, xt_ref, var_ref, varrow_ref, put, slots, pairs, fold)


def second_kernel(
    place_ref, near_ref, far_ref, x_ref, xt_ref, var_ref, varrow_ref, att_ref, wp_ref, mod_ref, wf_ref, wo_ref,
    mine_ref, send_ref,
    att_buf, res_buf, fin_buf, sum_buf,
    *, slots, pairs, channels, height, columns, halves, fold,
):
    group = place_ref[0]
    guide = place_ref[2]
    span = pairs * LANES
    first = pl.multiple_of(group * span, LANES) if halves == 2 else 0
    att_buf[:, pl.ds(first, span)] = att_ref[...]
    if halves == 2:
        other = (1 - group) * span

        def put(pair, value):
            at = pl.multiple_of(other + pair * LANES, LANES)
            att_buf[:, pl.ds(at, LANES)] = value

        attend_pairs(place_ref, near_ref, far_ref, x_ref, xt_ref, var_ref, varrow_ref, put, slots, pairs, fold)
    tokens = x_ref.shape[0]
    feats, model = wp_ref.shape
    x = x_ref[:, :feats]
    tiles = [(at, min(2 * LANES, model - at)) for at in range(0, model, 2 * LANES)]
    sum_buf[...] = jnp.zeros(sum_buf.shape, f32)

    def folded(value):
        total = value[:, :LANES]
        for at in range(LANES, value.shape[1], LANES):
            total = total + value[:, at : at + LANES]
        return total

    for at, size in tiles:
        cols = slice(at, at + size)
        mixed = dot(att_buf[...], wo_ref[:, cols])
        value = dot(x, wp_ref[:, cols]) + mod_ref[2, :, cols] * mixed
        res_buf[:, cols] = value
        sum_buf[...] = sum_buf[...] + folded(value)
    mean = jnp.sum(sum_buf[...], axis=1, keepdims=True) * (1.0 / model)
    sum_buf[...] = jnp.zeros(sum_buf.shape, f32)
    for at, size in tiles:
        cols = slice(at, at + size)
        value = res_buf[:, cols] - mean
        fin_buf[:, cols] = value.astype(bf16)
        sum_buf[...] = sum_buf[...] + folded(value * value)
    spread = jnp.sum(sum_buf[...], axis=1, keepdims=True) * (1.0 / model)
    result = dot(fin_buf[...], wf_ref[...], ((1,), (1,))) * lax.rsqrt(spread + epsilon)
    near = height // 2 + 1
    keep = guide * (near - 2)
    give = (1 - guide) * (near - 2)
    for p in range(height // 2):
        turned = result[p * columns : (p + 1) * columns].T
        for a in range(2):
            r = 2 * p + a
            for b in range(2):
                f = (a * 2 + b) * channels
                piece = turned[f : f + channels]

                @pl.when(jnp.logical_and(r >= keep, r < keep + near))
                def _():
                    mine_ref[r - keep, :, b * columns : (b + 1) * columns] = piece

                @pl.when(jnp.logical_and(r >= give, r < give + near))
                def _():
                    send_ref[r - give, :, b * columns : (b + 1) * columns] = piece.astype(bf16)


def spread_kernel(place_ref, mine_ref, theirs_ref, lat_ref, own_ref, one_ref, two_ref, back_ref):
    offset = place_ref[1]
    guide = place_ref[2]
    near, channels, wide = mine_ref.shape
    columns = wide // 2
    flat = near * channels
    first = guide * (near - 2)
    mine = mine_ref[...].reshape(flat, wide)
    theirs = theirs_ref[...].reshape(flat, wide).astype(f32)
    cond = jnp.where(guide == 0, mine, theirs)
    plain = jnp.where(guide == 0, theirs, mine)
    guided = plain + guidance * (cond - plain)
    high, low = split(guided)
    spot = iota((wide, 2 * columns), 0)
    lane = iota((wide, 2 * columns), 1)
    b = (spot >= columns).astype(jnp.int32)
    col = offset + 2 * (spot - b * columns) + b
    target = jnp.where(lane < columns, lane, jnp.where(lane == columns, -1, lane - 1))
    target = jnp.where(lane > columns + 1, -4 * wide, target)
    edge = iota((flat, columns), 1)

    def place(distance):
        return jnp.where(col == target + distance * columns, 1.0, 0.0).astype(bf16)

    def flagged(values, distance):
        for at, column in ((2, distance * columns - 1), (3, (distance + 1) * columns)):
            covered = jnp.logical_and(column >= offset, column < offset + wide)
            values = jnp.where(edge == at, jnp.where(covered, 1.0, 0.0), values)
        return values

    latent = jnp.concatenate(
        [lat_ref[:, pl.ds(first + i, 1), :].reshape(channels, columns) for i in range(near)], axis=0
    )
    top = latent.astype(bf16).astype(f32)
    middle = (latent - top).astype(bf16).astype(f32)
    bottom = latent - top - middle

    def border(values, column):
        for at, part in enumerate((top, middle, bottom)):
            moved = pltpu.roll(part, (4 + at - column) % columns, 1)
            values = jnp.where(edge == 4 + at, moved, values)
        return values

    here = place(0)
    own = dot(high, here) + dot(low, here)
    own_ref[:, :columns] = own[:, :columns]
    own_ref[:, columns:] = flagged(own[:, columns:], 0)
    one = dot(high, place(1))
    one_ref[:, :columns] = one[:, :columns].astype(bf16)
    one_ref[:, columns:] = border(flagged(one[:, columns:], 1), columns - 1).astype(bf16)
    two = dot(high, place(2))
    two_ref[:, :columns] = two[:, :columns].astype(bf16)
    two_ref[:, columns:] = flagged(two[:, columns:], 2).astype(bf16)
    back = dot(high, place(-1)[:, columns:])
    back_ref[...] = border(flagged(back, -1), 0).astype(bf16)


def decode_kernel(
    place_ref, own_ref, one_ref, two_ref, back_ref, lat_ref, count_ref, w_ref, den_ref, feat_ref, pad_buf,
    *, width,
):
    guide = place_ref[2]
    place = place_ref[3]
    channels, height, columns = lat_ref.shape
    half = height // 2
    near = half + 1
    flat = near * channels
    first = guide * (near - 2)
    fraction = (jnp.full((1, columns), place_ref[4], jnp.int32).astype(f32) + 1.0) / STEPS
    sigma = 3.0 * fraction / (1.0 + 2.0 * fraction)
    one = one_ref[...].astype(f32)
    back = back_ref[...].astype(f32)
    total = own_ref[...] + one + two_ref[...].astype(f32)
    latent = jnp.concatenate(
        [lat_ref[:, pl.ds(first + i, 1), :].reshape(channels, columns) for i in range(near)], axis=0
    )
    main = latent - sigma * (total[:, :columns] / count_ref[...].astype(f32))
    edges = total[:, columns:] + back
    left = one[:, columns + 4 : columns + 5] + one[:, columns + 5 : columns + 6] + one[:, columns + 6 : columns + 7]
    right = back[:, 4:5] + back[:, 5:6] + back[:, 6:7]
    left = left - sigma[:, :1] * (edges[:, 0:1] / edges[:, 2:3])
    right = right - sigma[:, :1] * (edges[:, 1:2] / edges[:, 3:4])
    left = jnp.where(place == 0, 0.0, left)
    right = jnp.where(place == width - 1, 0.0, right)
    lane = iota((flat, columns), 1)
    before = jnp.where(lane == 0, left, pltpu.roll(main, 1, 1))
    after = jnp.where(lane == columns - 1, right, pltpu.roll(main, columns - 1, 1))
    zero = jnp.zeros((channels, columns), f32)
    for b, value in enumerate((before, main, after)):
        pad_buf[b, 0] = zero
        pad_buf[b, near + 1] = zero
        for i in range(near):
            pad_buf[b, i + 1] = value[i * channels : (i + 1) * channels]
    for r in range(half):
        at = guide + r
        den_ref[:, r, :] = pad_buf[1, at + 1]
        stacked = jnp.concatenate(
            [pad_buf[b, at + a] for a in range(3) for b in range(3)], axis=0
        ).astype(bf16)
        summed = dot(stacked, w_ref[...], ((0,), (0,)))
        feat_ref[r] = (summed / (1.0 + jnp.exp(-summed))).astype(bf16)


def shift(x, by):
    peers = lax.axis_size("width")
    return lax.ppermute(x, "width", [(i, (i + by) % peers) for i in range(peers)])


def swap(x, axis):
    return lax.ppermute(x, axis, [(0, 1), (1, 0)])


def major_route(width, fold, d):
    return [(i, (i // fold ^ d) * fold + i % fold) for i in range(width)]


def gather_major(chunk, fold, direct):
    width = lax.axis_size("width")
    if not direct:
        every = lax.all_gather(chunk, "width")
        every = every.reshape((width // fold, fold) + chunk.shape)
        return lax.dynamic_index_in_dim(every, lax.axis_index("width") % fold, 1, False)
    pieces = [chunk]
    for d in range(1, width // fold):
        pieces.append(lax.ppermute(chunk, "width", major_route(width, fold, d)))
    return jnp.stack(pieces)


def swap_minor(stack, fold):
    if fold == 1:
        return stack
    width = lax.axis_size("width")
    return lax.ppermute(stack, "width", [(i, i ^ 1) for i in range(width)])


def shards(latent, starts, counts, step_index, cond_mod, w_patch, w_qkv, w_out, w_final, w_dec):
    guide = lax.axis_index("guide")
    place = lax.axis_index("width")
    group = lax.axis_index("groups")
    width = lax.axis_size("width")
    channels, height, columns = latent.shape
    model = w_patch.shape[1]
    feats = w_patch.shape[0]
    features = HEADS * HEAD
    pairs = features // LANES
    halves = 2 if lax.axis_size("groups") == 2 and pairs % 2 == 0 else 1
    local_pairs = pairs // halves
    slots = -(-3 * local_pairs // width)
    if halves == 1:
        group = group * 0
    rows = w_qkv.shape[0]
    fold = 2 if width % 2 == 0 else 1
    depth = width // fold
    direct = fold == 2 and depth <= 8 and depth & (depth - 1) == 0
    changes = jnp.swapaxes(cond_mod, 0, 1)
    offset = starts[0] - place * columns
    key = place // fold if direct else 0
    scalars = jnp.stack([group, offset, guide, place, step_index[0], key]).astype(jnp.int32)

    right = shift(latent, -1)
    further = shift(latent, -2)

    slab = (ROWS, slots * LANES)
    in_hbm = functools.partial(pltpu.with_memory_space_constraint, memory_space=pltpu.HBM)
    parts = call(
        functools.partial(
            partial_kernel, width=width, slots=slots, local_pairs=local_pairs, features=features,
            fold=fold, direct=direct,
        ),
        [((depth,) + slab, f32), ((depth,) + slab, bf16)] if direct else [((width,) + slab, bf16)],
        scratch=[
            pltpu.VMEM((3, rows, local_pairs * LANES), bf16),
            pltpu.VMEM(changes.shape, f32),
            pltpu.VMEM(w_patch.shape, bf16),
            pltpu.SemaphoreType.DMA((5,)),
        ],
        anys=(1, 2, 3), smem=(0,), count=4, limit=8,
    )(scalars, in_hbm(changes), in_hbm(w_patch), in_hbm(w_qkv))
    near = height // 2 + 1
    tokens = height // 2 * columns
    if direct:
        came = swap_minor(parts[1], fold)
    else:
        came = lax.all_to_all(parts[0], "width", 0, 0, tiled=True)
    x, xt, var, varrow = call(
        window_kernel,
        [((tokens, LANES), bf16), ((ROWS, tokens), bf16), ((tokens, LANES), f32), ((8, tokens), f32)],
        scratch=[
            pltpu.VMEM((height * channels, 3 * columns), bf16),
            pltpu.VMEM((feats, tokens), f32),
            pltpu.VMEM((tokens, model), f32),
            pltpu.VMEM(w_patch.shape, bf16),
            pltpu.SemaphoreType.DMA((1,)),
        ],
        anys=(4,), smem=(0,), count=5, flops=5e9,
    )(scalars, latent, right, further, in_hbm(w_patch))
    came, x = lax.optimization_barrier((came, x))
    if direct:
        own, *sends = call(
            first_sum_kernel, [(slab, f32)] + [(slab, bf16)] * (depth - 1), smem=(0,), count=3, limit=4
        )(scalars, parts[0], came)
        got = [lax.ppermute(v, "width", major_route(width, fold, d + 1)) for d, v in enumerate(sends)]
        (chunk,) = call(last_sum_kernel, [(slab, bf16)], count=depth, limit=4)(own, *got)
    else:
        (chunk,) = call(
            functools.partial(sum_kernel, width=width), [(slab, bf16)], count=1, limit=4
        )(came)
    stack = gather_major(chunk, fold, direct)
    side = swap_minor(stack, fold)
    if halves == 2:
        stack_x, side_x = swap(stack, "groups"), swap(side, "groups")
    else:
        stack_x, side_x = stack, side
    (att,) = call(
        functools.partial(first_kernel, slots=slots, pairs=local_pairs, fold=fold),
        [((tokens, local_pairs * LANES), bf16)],
        smem=(0,), count=7, flops=6e9,
    )(scalars, stack, side, x, xt, var, varrow)
    mine_v, send_v = call(
        functools.partial(
            second_kernel, slots=slots, pairs=local_pairs, channels=channels, height=height,
            columns=columns, halves=halves, fold=fold,
        ),
        [((near, channels, 2 * columns), f32), ((near, channels, 2 * columns), bf16)],
        scratch=[
            pltpu.VMEM((tokens, features), bf16),
            pltpu.VMEM((tokens, model), f32),
            pltpu.VMEM((tokens, model), bf16),
            pltpu.VMEM((tokens, LANES), f32),
        ],
        smem=(0,), count=12, flops=12e9, limit=22,
    )(scalars, stack_x, side_x, x, xt, var, varrow, att, w_patch, changes, w_final.T, w_out)
    theirs = swap(send_v, "guide")
    flat = near * channels
    own, one, two, back = call(
        spread_kernel,
        [
            ((flat, 2 * columns), f32), ((flat, 2 * columns), bf16),
            ((flat, 2 * columns), bf16), ((flat, columns), bf16),
        ],
        smem=(0,), count=4, limit=8,
    )(scalars, mine_v, theirs, latent)
    one = shift(one, 1)
    two = shift(two, 2)
    back = shift(back, -1)
    return call(
        functools.partial(decode_kernel, width=width),
        [((channels, height // 2, columns), f32), ((height // 2, columns, w_dec.shape[1]), bf16)],
        scratch=[pltpu.VMEM((3, near + 2, channels, columns), f32)],
        smem=(0,), count=8, limit=8,
    )(scalars, own, one, two, back, latent, counts[None], w_dec)


def solution(mesh):
    return jax.shard_map(
        shards,
        mesh=mesh,
        in_specs=(
            P(None, None, ("groups", "width")),
            P(("groups", "width")),
            P(("groups", "width")),
            P("groups"),
            P("guide", None, None),
            P(),
            P("width", None),
            P(),
            P(),
            P(),
        ),
        out_specs=(P(None, "guide", ("groups", "width")), P("guide", ("groups", "width"), None)),
        check_vma=False,
    )
```

```python
import functools

import jax
import jax.numpy as jnp
from jax import lax
from jax.experimental import pallas as pl
from jax.experimental.pallas import tpu as pltpu
from jax.sharding import PartitionSpec as P


HEADS = 20
HEAD = 64
STEPS = 28
LANES = 128
ROWS = 72

guidance = 4.0
epsilon = 1e-06

bf16 = jnp.bfloat16
f32 = jnp.float32
PARTS = (0, 2, 1)
LOG2E = 1.4426950408889634


def dot(a, b, dims=((1,), (0,))):
    return lax.dot_general(a, b, (dims, ((), ())), preferred_element_type=f32)


def call(body, outs, scratch=(), anys=(), smem=(), count=0, limit=16, flops=0):
    def spec(i):
        if i in anys:
            return pl.BlockSpec(memory_space=pltpu.HBM)
        if i in smem:
            return pl.BlockSpec(memory_space=pltpu.SMEM)
        return pl.BlockSpec(memory_space=pltpu.VMEM)

    return pl.pallas_call(
        body,
        out_shape=tuple(jax.ShapeDtypeStruct(s, t) for s, t in outs),
        in_specs=[spec(i) for i in range(count)],
        out_specs=tuple(pl.BlockSpec(memory_space=pltpu.VMEM) for _ in outs),
        scratch_shapes=list(scratch),
        compiler_params=pltpu.CompilerParams(vmem_limit_bytes=limit << 20),
        cost_estimate=pl.CostEstimate(flops=int(flops), bytes_accessed=1 << 20, transcendentals=0),
    )


def iota(shape, dim):
    return lax.broadcasted_iota(jnp.int32, shape, dim)


def layout(local_pairs, depth, slots, fold):
    whole = local_pairs // fold
    sides = [[(y * whole + j, sub) for j in range(whole) for sub in range(3)] for y in range(fold)]
    for pair in range(fold * whole, local_pairs):
        for sub in range(3):
            y = next(y for y in range(fold) if len(sides[y]) < depth * slots)
            sides[y].append((pair, sub))
    return whole, sides


def split(values):
    high = values.astype(bf16)
    return high, (values - high.astype(f32)).astype(bf16)


def partial_kernel(
    place_ref, mod_ref, wp_ref, w_ref, *refs, width, slots, local_pairs, features, fold, direct
):
    *out_refs, w_buf, mod_buf, wp_buf, sems = refs
    group = place_ref[0]
    span = local_pairs * LANES
    loads = [
        pltpu.make_async_copy(wp_ref, wp_buf, sems.at[0]),
        pltpu.make_async_copy(mod_ref, mod_buf, sems.at[1]),
    ]
    for part in range(3):
        start = pl.multiple_of(part * features + group * span, LANES)
        loads.append(
            pltpu.make_async_copy(w_ref.at[:, pl.ds(start, span)], w_buf.at[part], sems.at[2 + part])
        )
    for one in loads:
        one.start()
    feats, model = wp_ref.shape
    rows = w_buf.shape[1]
    window = min(model, -(-(rows + LANES - 1) // LANES) * LANES)
    begin = place_ref[2] * rows
    low = jnp.minimum(begin // LANES * LANES, model - window)
    cols = pl.ds(pl.multiple_of(low, LANES), window)
    loads[0].wait()
    loads[1].wait()
    mean = jnp.sum(wp_buf[...].astype(f32), axis=1, keepdims=True) * (1.0 / model)
    centered = wp_buf[:, cols].astype(f32) - mean
    scaled = centered * (1.0 + mod_buf[1, :, cols])
    down = iota((ROWS - feats, window), 0)
    tail = jnp.where(down < 2, jnp.broadcast_to(mod_buf[0, :, cols], down.shape), 0.0)
    stacked = jnp.concatenate([scaled, tail], axis=0)
    stacked = pltpu.roll(stacked, (window - (begin - low)) % window, 1)
    a = jnp.concatenate(split(stacked), axis=0)[:, :rows]
    for one in loads[2:]:
        one.wait()
    side = place_ref[2] % fold
    _, sides = layout(local_pairs, width // fold, slots, fold)
    for owner in range(width):
        z, y = divmod(owner, fold)
        pieces = []
        for slot in range(slots):
            spot = z * slots + slot
            if spot < len(sides[y]):
                pair, sub = sides[y][spot]
                both = dot(a, w_buf[PARTS[sub], :, pair * LANES : (pair + 1) * LANES])
                pieces.append(both[:ROWS] + both[ROWS:])
            else:
                pieces.append(jnp.zeros((ROWS, LANES), f32))
        value = jnp.concatenate(pieces, axis=1)
        if not direct:
            out_refs[0][owner] = value.astype(bf16)
            continue

        @pl.when(side == y)
        def _():
            out_refs[0][z] = value

        @pl.when(side != y)
        def _():
            out_refs[1][z] = value.astype(bf16)


def sum_kernel(parts_ref, out_ref, *, width):
    total = parts_ref[0].astype(f32)
    for i in range(1, width):
        total = total + parts_ref[i].astype(f32)
    out_ref[...] = total.astype(bf16)


def first_sum_kernel(place_ref, keep_ref, came_ref, own_ref, *send_refs):
    key = place_ref[3]
    own_ref[...] = keep_ref[key] + came_ref[key].astype(f32)
    for d, ref in enumerate(send_refs):
        at = key ^ (d + 1)
        ref[...] = (keep_ref[at] + came_ref[at].astype(f32)).astype(bf16)


def last_sum_kernel(*refs):
    *parts, out_ref = refs
    total = parts[0][...]
    for ref in parts[1:]:
        total = total + ref[...].astype(f32)
    out_ref[...] = total.astype(bf16)


def window_kernel(
    place_ref, start_ref, own_ref, right_ref, further_ref, wp_ref,
    x_ref, xt_ref, var_ref, varrow_ref, hid_ref,
    rows_buf, xt_buf, w_ref, sem,
):
    load = pltpu.make_async_copy(wp_ref, w_ref, sem.at[0])
    load.start()
    channels, height, columns = own_ref.shape
    offset = start_ref[0] - place_ref[2] * columns
    for r in range(height):
        at = slice(r * channels, (r + 1) * channels)
        rows_buf[at, :columns] = own_ref[:, r, :].astype(bf16)
        rows_buf[at, columns : 2 * columns] = right_ref[:, r, :].astype(bf16)
        rows_buf[at, 2 * columns :] = further_ref[:, r, :].astype(bf16)
    col = iota((3 * columns, 2 * columns), 0)
    spot = iota((3 * columns, 2 * columns), 1)
    b = (spot >= columns).astype(jnp.int32)
    pick = jnp.where(col == offset + 2 * (spot - b * columns) + b, 1.0, 0.0).astype(bf16)
    placed = dot(rows_buf[...], pick).astype(bf16)
    tokens = height // 2 * columns
    for p in range(height // 2):
        for a in range(2):
            for b in range(2):
                f = (a * 2 + b) * channels
                xt_buf[f : f + channels, p * columns : (p + 1) * columns] = placed[
                    (2 * p + a) * channels : (2 * p + a + 1) * channels, b * columns : (b + 1) * columns
                ].astype(f32)
    feats = 4 * channels
    xt = xt_buf[:feats, :]
    xpad = jnp.concatenate([xt, jnp.zeros((LANES - feats, tokens), f32)], axis=0)
    xrow = xpad.T
    model = w_ref.shape[1]
    block = 64
    x_bf = xrow[:, :feats].astype(bf16)
    load.wait()
    hid_ref[...] = dot(x_bf, w_ref[...])

    def stats(i, carry):
        at = pl.ds(pl.multiple_of(i * block, block), block)
        h = hid_ref[at, :]
        mean = jnp.sum(h, axis=1, keepdims=True) * (1.0 / model)
        c = h - mean
        v = jnp.sum(c * c, axis=1, keepdims=True) * (1.0 / model)
        var_ref[at, :] = jnp.broadcast_to(v, (block, LANES))
        return carry

    lax.fori_loop(0, tokens // block, stats, 0)
    var = var_ref[...]
    std_hi, std_lo = split(jnp.sqrt(var + epsilon))
    spots = iota((tokens, LANES), 1)
    x_ref[...] = jnp.where(
        spots == feats, std_hi.astype(f32), jnp.where(spots == feats + 1, std_lo.astype(f32), xrow)
    ).astype(bf16)
    var_t = var.T[:8]
    varrow_ref[...] = var_t
    hi_t, lo_t = split(jnp.sqrt(var_t + epsilon))
    down = iota((8, tokens), 0)
    tail = jnp.where(down == 0, hi_t.astype(f32), jnp.where(down == 1, lo_t.astype(f32), 0.0))
    xt_ref[...] = jnp.concatenate([xt, tail], axis=0).astype(bf16)


def attend_units(place_ref, near_ref, far_ref, x_ref, xt_ref, var_ref, varrow_ref, put, units, slots, pairs, fold):
    tokens = x_ref.shape[0]
    key = place_ref[3]
    side = place_ref[2] % fold
    whole, sides = layout(pairs, near_ref.shape[0], slots, fold)
    x = x_ref[:, :ROWS]
    scale = LOG2E * HEAD**-0.5

    def tile(unit, sub):
        far = jnp.logical_and(unit >= whole, unit < fold * whole)
        spot = 3 * (unit - jnp.where(far, whole, 0)) + sub
        for pair in range(fold * whole, pairs):
            y = next(y for y in range(fold) if (pair, sub) in sides[y])
            mine = unit == pair
            far = jnp.where(mine, side != y, far)
            spot = jnp.where(mine, sides[y].index((pair, sub)), spot)
        at = (
            (spot // slots) ^ key,
            slice(None),
            pl.ds(pl.multiple_of(spot % slots * LANES, LANES), LANES),
        )
        return jnp.where(far, far_ref[at], near_ref[at])

    def one(unit, carry):
        mq, mv, mk = (tile(unit, sub) for sub in range(3))
        low = iota((tokens, LANES), 1) < HEAD
        var = var_ref[...]
        both = dot(x, jnp.concatenate([mq, mv], axis=1))
        uq = both[:, :LANES]
        uv = both[:, LANES:] * lax.rsqrt(var + epsilon)
        uk = dot(mk, xt_ref[...], ((0,), (0,)))
        sq = uq * uq
        sum_low = jnp.sum(jnp.where(low, sq, 0.0), axis=1, keepdims=True)
        sum_high = jnp.sum(jnp.where(low, 0.0, sq), axis=1, keepdims=True)
        mean = jnp.where(low, sum_low, sum_high) * (1.0 / HEAD)
        q = uq * lax.rsqrt(mean + epsilon * (var + epsilon))
        eps_row = epsilon * (varrow_ref[:1, :] + epsilon)
        keys = []
        for half in range(2):
            k = uk[half * HEAD : (half + 1) * HEAD]
            mean = jnp.sum(k * k, axis=0, keepdims=True) * (1.0 / HEAD)
            keys.append((k * lax.rsqrt(mean + eps_row)).astype(bf16))
        kt = jnp.concatenate(keys, axis=0)
        outs = []
        for half in range(2):
            mine = low if half == 0 else jnp.logical_not(low)
            qh = jnp.where(mine, q, 0.0).astype(bf16)
            vh = jnp.where(mine, uv, 1.0).astype(bf16)
            weights = jnp.exp2(dot(qh, kt) * scale).astype(bf16)
            outs.append(dot(weights, vh))
        top = jnp.where(low, outs[0], outs[1])
        sums = pltpu.roll(jnp.where(low, outs[1], outs[0]), HEAD, 1)
        put(unit, (top / sums).astype(bf16))
        return carry

    lax.fori_loop(*units, one, 0)


def attend_kernel(
    place_ref, near_ref, far_ref, x_ref, xt_ref, var_ref, varrow_ref, att_ref, *, units, slots, pairs, fold
):
    def put(unit, value):
        att_ref[:, pl.ds(pl.multiple_of((unit - units[0]) * LANES, LANES), LANES)] = value

    attend_units(
        place_ref, near_ref, far_ref, x_ref, xt_ref, var_ref, varrow_ref, put, units, slots, pairs, fold
    )


def near_kernel(place_ref, near_ref, x_ref, xt_ref, var_ref, varrow_ref, att_ref, **sizes):
    attend_kernel(place_ref, near_ref, near_ref, x_ref, xt_ref, var_ref, varrow_ref, att_ref, **sizes)


def second_kernel(
    place_ref, near_ref, far_ref, x_ref, xt_ref, var_ref, varrow_ref, hid_ref, mod_ref, wf_ref, wo_ref, *refs,
    slots, pairs, channels, height, columns, halves, fold, whole,
):
    *att_refs, mine_ref, send_ref, att_buf, res_buf, fin_buf, sum_buf = refs
    group = place_ref[0]
    guide = place_ref[1]
    side = place_ref[2] % fold

    def lanes(half, unit):
        far = jnp.logical_and(unit >= whole, unit < fold * whole)
        at = jnp.where(far, unit - whole + (1 - side) * whole, unit + side * whole)
        at = jnp.where(unit >= fold * whole, unit, at) + half * pairs
        return pl.ds(pl.multiple_of(at * LANES, LANES), LANES)

    unit = 0
    for ref in att_refs:
        for at in range(0, ref.shape[1], LANES):
            att_buf[:, lanes(group, unit)] = ref[:, at : at + LANES]
            unit += 1
    if halves == 2:

        def put(unit, value):
            att_buf[:, lanes(1 - group, unit)] = value

        attend_units(
            place_ref, near_ref, far_ref, x_ref, xt_ref, var_ref, varrow_ref, put, (0, pairs), slots, pairs, fold
        )
    _, model = hid_ref.shape
    sum_buf[...] = jnp.zeros(sum_buf.shape, f32)

    def folded(value):
        total = value[:, :LANES]
        for at in range(LANES, value.shape[1], LANES):
            total = total + value[:, at : at + LANES]
        return total

    def project(cols):
        mixed = dot(att_buf[...], wo_ref[:, cols])
        value = hid_ref[:, cols] + mod_ref[2, :, cols] * mixed
        res_buf[:, cols] = value
        sum_buf[...] = sum_buf[...] + folded(value)

    def sweep(step):
        size = 2 * LANES

        def body(i, carry):
            step(pl.ds(pl.multiple_of(i * size, LANES), size))
            return carry

        lax.fori_loop(0, model // size, body, 0)
        if model % size:
            step(slice(model // size * size, model))

    sweep(project)
    mean = jnp.sum(sum_buf[...], axis=1, keepdims=True) * (1.0 / model)
    sum_buf[...] = jnp.zeros(sum_buf.shape, f32)

    def center(cols):
        value = res_buf[:, cols] - mean
        fin_buf[:, cols] = value.astype(bf16)
        sum_buf[...] = sum_buf[...] + folded(value * value)

    sweep(center)
    spread = jnp.sum(sum_buf[...], axis=1, keepdims=True) * (1.0 / model)
    result = dot(fin_buf[...], wf_ref[...], ((1,), (1,))) * lax.rsqrt(spread + epsilon)
    near = height // 2 + 1
    keep = guide * (near - 2)
    give = (1 - guide) * (near - 2)
    for p in range(height // 2):
        turned = result[p * columns : (p + 1) * columns].T
        for a in range(2):
            r = 2 * p + a
            for b in range(2):
                f = (a * 2 + b) * channels
                piece = turned[f : f + channels]

                @pl.when(jnp.logical_and(r >= keep, r < keep + near))
                def _():
                    mine_ref[r - keep, :, b * columns : (b + 1) * columns] = piece

                @pl.when(jnp.logical_and(r >= give, r < give + near))
                def _():
                    send_ref[r - give, :, b * columns : (b + 1) * columns] = piece.astype(bf16)


def spread_kernel(
    place_ref, start_ref, mine_ref, theirs_ref, lat_ref, own_ref, odd_ref, two_ref, even_ref
):
    guide = place_ref[1]
    place = place_ref[2]
    near, channels, wide = mine_ref.shape
    columns = wide // 2
    offset = start_ref[0] - place * columns
    flat = near * channels
    first = guide * (near - 2)
    mine = mine_ref[...].reshape(flat, wide)
    theirs = theirs_ref[...].reshape(flat, wide).astype(f32)
    cond = jnp.where(guide == 0, mine, theirs)
    plain = jnp.where(guide == 0, theirs, mine)
    guided = plain + guidance * (cond - plain)
    high, low = split(guided)
    spot = iota((wide, 2 * columns), 0)
    lane = iota((wide, 2 * columns), 1)
    b = (spot >= columns).astype(jnp.int32)
    col = offset + 2 * (spot - b * columns) + b
    target = jnp.where(lane < columns, lane, jnp.where(lane == columns, -1, lane - 1))
    target = jnp.where(lane > columns + 1, -4 * wide, target)
    edge = iota((flat, columns), 1)

    def spots(distance):
        return jnp.where(col == target + distance * columns, 1.0, 0.0).astype(bf16)

    def flagged(values, distance):
        for at, column in ((2, distance * columns - 1), (3, (distance + 1) * columns)):
            covered = jnp.logical_and(column >= offset, column < offset + wide)
            values = jnp.where(edge == at, jnp.where(covered, 1.0, 0.0), values)
        return values

    latent = jnp.concatenate(
        [lat_ref[:, pl.ds(first + i, 1), :].reshape(channels, columns) for i in range(near)], axis=0
    )
    top = latent.astype(bf16).astype(f32)
    middle = (latent - top).astype(bf16).astype(f32)
    bottom = latent - top - middle

    def border(values, column):
        for at, part in enumerate((top, middle, bottom)):
            moved = pltpu.roll(part, (4 + at - column) % columns, 1)
            values = jnp.where(edge == 4 + at, moved, values)
        return values

    here = spots(0)
    own = dot(high, here) + dot(low, here)
    own_ref[:, :columns] = own[:, :columns]
    own_ref[:, columns:] = flagged(own[:, columns:], 0)
    one = dot(high, spots(1))
    one_edge = border(flagged(one[:, columns:], 1), columns - 1)
    two = dot(high, spots(2))
    two_ref[:, :columns] = two[:, :columns].astype(bf16)
    two_ref[:, columns:] = flagged(two[:, columns:], 2).astype(bf16)
    back = dot(high, spots(-1)[:, columns:])
    back_edge = border(flagged(back, -1), 0)
    odd = place % 2 == 1
    odd_ref[:, :columns] = one[:, :columns].astype(bf16)
    even_ref[:, :columns] = one[:, :columns].astype(bf16)
    odd_ref[:, columns:] = jnp.where(odd, one_edge, back_edge).astype(bf16)
    even_ref[:, columns:] = jnp.where(odd, back_edge, one_edge).astype(bf16)


def decode_kernel(
    place_ref, step_ref, own_ref, odd_ref, two_ref, even_ref, lat_ref, count_ref, w_ref, den_ref, feat_ref, pad_buf,
    *, width,
):
    guide = place_ref[1]
    place = place_ref[2]
    channels, height, columns = lat_ref.shape
    half = height // 2
    near = half + 1
    flat = near * channels
    first = guide * (near - 2)
    fraction = (jnp.full((1, columns), step_ref[0], jnp.int32).astype(f32) + 1.0) / STEPS
    sigma = 3.0 * fraction / (1.0 + 2.0 * fraction)
    odd = place % 2 == 1
    one = jnp.where(odd, even_ref[...], odd_ref[...]).astype(f32)
    back = jnp.where(odd, odd_ref[:, columns:], even_ref[:, columns:]).astype(f32)
    total = own_ref[...] + one + two_ref[...].astype(f32)
    latent = jnp.concatenate(
        [lat_ref[:, pl.ds(first + i, 1), :].reshape(channels, columns) for i in range(near)], axis=0
    )
    main = latent - sigma * (total[:, :columns] / count_ref[...].astype(f32))
    edges = total[:, columns:] + back
    left = one[:, columns + 4 : columns + 5] + one[:, columns + 5 : columns + 6] + one[:, columns + 6 : columns + 7]
    right = back[:, 4:5] + back[:, 5:6] + back[:, 6:7]
    left = left - sigma[:, :1] * (edges[:, 0:1] / edges[:, 2:3])
    right = right - sigma[:, :1] * (edges[:, 1:2] / edges[:, 3:4])
    left = jnp.where(place == 0, 0.0, left)
    right = jnp.where(place == width - 1, 0.0, right)
    lane = iota((flat, columns), 1)
    before = jnp.where(lane == 0, left, pltpu.roll(main, 1, 1))
    after = jnp.where(lane == columns - 1, right, pltpu.roll(main, columns - 1, 1))
    zero = jnp.zeros((channels, columns), f32)
    for b, value in enumerate((before, main, after)):
        pad_buf[b, 0] = zero
        pad_buf[b, near + 1] = zero
        for i in range(near):
            pad_buf[b, i + 1] = value[i * channels : (i + 1) * channels]
    for r in range(half):
        at = guide + r
        den_ref[:, r, :] = pad_buf[1, at + 1]
        stacked = jnp.concatenate(
            [pad_buf[b, at + a] for a in range(3) for b in range(3)], axis=0
        ).astype(bf16)
        summed = dot(stacked, w_ref[...], ((0,), (0,)))
        feat_ref[r] = (summed / (1.0 + jnp.exp(-summed))).astype(bf16)


def shift(x, by):
    peers = lax.axis_size("width")
    return lax.ppermute(x, "width", [(i, (i + by) % peers) for i in range(peers)])


def swap(x, axis):
    return lax.ppermute(x, axis, [(0, 1), (1, 0)])


def spread_major(pieces, fold):
    width = lax.axis_size("width")
    got = []
    for d in range(len(pieces), 0, -1):
        route = [(i, (i // fold ^ d) * fold + i % fold) for i in range(width)]
        got.append(lax.ppermute(pieces[d - 1], "width", route))
    return got[::-1]


def gather_major(chunk, fold, direct):
    width = lax.axis_size("width")
    depth = width // fold
    if not direct:
        every = lax.all_gather(chunk, "width")
        every = every.reshape((depth, fold) + chunk.shape)
        return lax.dynamic_index_in_dim(every, lax.axis_index("width") % fold, 1, False)
    return jnp.stack([chunk] + spread_major([chunk] * (depth - 1), fold))


def swap_minor(stack):
    width = lax.axis_size("width")
    return lax.ppermute(stack, "width", [(i, i ^ 1) for i in range(width)])


def shards(latent, starts, counts, step_index, cond_mod, w_patch, w_qkv, w_out, w_final, w_dec):
    guide = lax.axis_index("guide")
    place = lax.axis_index("width")
    group = lax.axis_index("groups")
    width = lax.axis_size("width")
    channels, height, columns = latent.shape
    model = w_patch.shape[1]
    feats = w_patch.shape[0]
    features = HEADS * HEAD
    pairs = features // LANES
    halves = 2 if lax.axis_size("groups") == 2 and pairs % 2 == 0 else 1
    local_pairs = pairs // halves
    slots = -(-3 * local_pairs // width)
    if halves == 1:
        group = group * 0
    rows = w_qkv.shape[0]
    fold = 2
    depth = width // fold
    direct = depth <= 8 and depth & (depth - 1) == 0
    changes = jnp.swapaxes(cond_mod, 0, 1)
    key = place // fold if direct else 0
    scalars = jnp.stack([group, guide, place, key]).astype(jnp.int32)

    right = shift(latent, -1)
    further = shift(latent, -2)

    slab = (ROWS, slots * LANES)
    in_hbm = functools.partial(pltpu.with_memory_space_constraint, memory_space=pltpu.HBM)
    parts = call(
        functools.partial(
            partial_kernel, width=width, slots=slots, local_pairs=local_pairs, features=features,
            fold=fold, direct=direct,
        ),
        [((depth,) + slab, f32), ((depth,) + slab, bf16)] if direct else [((width,) + slab, bf16)],
        scratch=[
            pltpu.VMEM((3, rows, local_pairs * LANES), bf16),
            pltpu.VMEM(changes.shape, f32),
            pltpu.VMEM(w_patch.shape, bf16),
            pltpu.SemaphoreType.DMA((5,)),
        ],
        anys=(1, 2, 3), smem=(0,), count=4, limit=8,
    )(scalars, in_hbm(changes), in_hbm(w_patch), in_hbm(w_qkv))
    near = height // 2 + 1
    tokens = height // 2 * columns
    if direct:
        came = swap_minor(parts[1])
    else:
        came = lax.all_to_all(parts[0], "width", 0, 0, tiled=True)
    x, xt, var, varrow, hidden = call(
        window_kernel,
        [
            ((tokens, LANES), bf16), ((ROWS, tokens), bf16), ((tokens, LANES), f32), ((8, tokens), f32),
            ((tokens, model), f32),
        ],
        scratch=[
            pltpu.VMEM((height * channels, 3 * columns), bf16),
            pltpu.VMEM((feats, tokens), f32),
            pltpu.VMEM(w_patch.shape, bf16),
            pltpu.SemaphoreType.DMA((1,)),
        ],
        anys=(5,), smem=(0, 1), count=6, flops=5e9,
    )(scalars, starts, latent, right, further, in_hbm(w_patch))
    came, x = lax.optimization_barrier((came, x))
    if direct:
        own, *sends = call(
            first_sum_kernel, [(slab, f32)] + [(slab, bf16)] * (depth - 1), smem=(0,), count=3, limit=4
        )(scalars, parts[0], came)
        got = spread_major(sends, fold)
        (chunk,) = call(last_sum_kernel, [(slab, bf16)], count=depth, limit=4)(own, *got)
    else:
        (chunk,) = call(
            functools.partial(sum_kernel, width=width), [(slab, bf16)], count=1, limit=4
        )(came)
    stack = gather_major(chunk, fold, direct)
    side = swap_minor(stack)
    stack_x = swap(stack, "groups") if halves == 2 else stack
    whole = local_pairs // fold
    sizes = dict(slots=slots, pairs=local_pairs, fold=fold)
    (att_near,) = call(
        functools.partial(near_kernel, units=(0, whole), **sizes),
        [((tokens, whole * LANES), bf16)],
        smem=(0,), count=6, flops=2e9,
    )(scalars, stack, x, xt, var, varrow)
    side, att_near = lax.optimization_barrier((side, att_near))
    if halves == 2:
        side_x = swap(side, "groups")
    else:
        side_x = side
    (att_far,) = call(
        functools.partial(attend_kernel, units=(whole, local_pairs), **sizes),
        [((tokens, (local_pairs - whole) * LANES), bf16)],
        smem=(0,), count=7, flops=3e9,
    )(scalars, stack, side, x, xt, var, varrow)
    mine_v, send_v = call(
        functools.partial(
            second_kernel, channels=channels, height=height, columns=columns, halves=halves, whole=whole, **sizes
        ),
        [((near, channels, 2 * columns), f32), ((near, channels, 2 * columns), bf16)],
        scratch=[
            pltpu.VMEM((tokens, features), bf16),
            pltpu.VMEM((tokens, model), f32),
            pltpu.VMEM((tokens, model), bf16),
            pltpu.VMEM((tokens, LANES), f32),
        ],
        smem=(0,), count=13, flops=12e9, limit=22,
    )(scalars, stack_x, side_x, x, xt, var, varrow, hidden, changes, w_final.T, w_out, att_near, att_far)
    theirs = swap(send_v, "guide")
    flat = near * channels
    own, odd, two, even = call(
        spread_kernel,
        [
            ((flat, 2 * columns), f32), ((flat, 2 * columns), bf16),
            ((flat, 2 * columns), bf16), ((flat, 2 * columns), bf16),
        ],
        smem=(0, 1), count=5, limit=8,
    )(scalars, starts, mine_v, theirs, latent)
    ups = [(i, (i + 1) % width) for i in range(width)]
    turns = [[pair for pair in ups if pair[0] % 2 == side] for side in range(2)]
    turns = [pairs + [(b, a) for a, b in pairs] for pairs in turns]
    odd = lax.ppermute(odd, "width", turns[1])
    two = lax.ppermute(two, "width", [(i, (i + 2) % width) for i in range(width)])
    even = lax.ppermute(even, "width", turns[0])
    return call(
        functools.partial(decode_kernel, width=width),
        [((channels, height // 2, columns), f32), ((height // 2, columns, w_dec.shape[1]), bf16)],
        scratch=[pltpu.VMEM((3, near + 2, channels, columns), f32)],
        smem=(0, 1), count=9, limit=8,
    )(scalars, step_index, own, odd, two, even, latent, counts[None], w_dec)


def solution(mesh):
    return jax.shard_map(
        shards,
        mesh=mesh,
        in_specs=(
            P(None, None, ("groups", "width")),
            P(("groups", "width")),
            P(("groups", "width")),
            P("groups"),
            P("guide", None, None),
            P(),
            P("width", None),
            P(),
            P(),
            P(),
        ),
        out_specs=(P(None, "guide", ("groups", "width")), P("guide", ("groups", "width"), None)),
        check_vma=False,
    )
```

```python
import functools

import jax
import jax.numpy as jnp
from jax import lax
from jax.experimental import pallas as pl
from jax.experimental.pallas import tpu as pltpu
from jax.sharding import PartitionSpec as P


HEADS = 20
HEAD = 64
STEPS = 28
LANES = 128
ROWS = 72


guidance = 4.0
epsilon = 1e-06

bf16 = jnp.bfloat16
f32 = jnp.float32
PARTS = (0, 2, 1)
LOG2E = 1.4426950408889634


def dot(a, b, dims=((1,), (0,))):
    return lax.dot_general(a, b, (dims, ((), ())), preferred_element_type=f32)


def call(body, outs, scratch=(), anys=(), smem=(), count=0, limit=16, flops=0, hbm_outs=()):
    def spec(i):
        if i in anys:
            return pl.BlockSpec(memory_space=pltpu.HBM)
        if i in smem:
            return pl.BlockSpec(memory_space=pltpu.SMEM)
        return pl.BlockSpec(memory_space=pltpu.VMEM)

    return pl.pallas_call(
        body,
        out_shape=tuple(jax.ShapeDtypeStruct(s, t) for s, t in outs),
        in_specs=[spec(i) for i in range(count)],
        out_specs=tuple(
            pl.BlockSpec(memory_space=pltpu.HBM if i in hbm_outs else pltpu.VMEM) for i in range(len(outs))
        ),
        scratch_shapes=list(scratch),
        compiler_params=pltpu.CompilerParams(vmem_limit_bytes=limit << 20),
        cost_estimate=pl.CostEstimate(flops=int(flops), bytes_accessed=1 << 20, transcendentals=0),
    )


def iota(shape, dim):
    return lax.broadcasted_iota(jnp.int32, shape, dim)


def layout(local_pairs, depth, slots, fold):
    whole = local_pairs // fold
    sides = [[(y * whole + j, sub) for j in range(whole) for sub in range(3)] for y in range(fold)]
    for pair in range(fold * whole, local_pairs):
        for sub in range(3):
            y = next(y for y in range(fold) if len(sides[y]) < depth * slots)
            sides[y].append((pair, sub))
    return whole, sides


def split(values):
    high = values.astype(bf16)
    return high, (values - high.astype(f32)).astype(bf16)


def partial_kernel(
    place_ref, mod_ref, wp_ref, w_ref, *refs, width, slots, local_pairs, features, fold, direct
):
    *out_refs, w_buf, mod_buf, wp_buf, all_buf, sems = refs
    group = place_ref[0]
    span = local_pairs * LANES
    loads = [
        pltpu.make_async_copy(wp_ref, wp_buf, sems.at[0]),
        pltpu.make_async_copy(mod_ref, mod_buf, sems.at[1]),
    ]
    for part in range(3):
        start = pl.multiple_of(part * features + group * span, LANES)
        loads.append(
            pltpu.make_async_copy(w_ref.at[:, pl.ds(start, span)], w_buf.at[part], sems.at[2 + part])
        )
    for one in loads:
        one.start()
    feats, model = wp_ref.shape
    rows = w_buf.shape[1]
    window = min(model, -(-(rows + LANES - 1) // LANES) * LANES)
    begin = place_ref[2] * rows
    low = jnp.minimum(begin // LANES * LANES, model - window)
    cols = pl.ds(pl.multiple_of(low, LANES), window)
    loads[0].wait()
    loads[1].wait()
    mean = jnp.sum(wp_buf[...].astype(f32), axis=1, keepdims=True) * (1.0 / model)
    centered = wp_buf[:, cols].astype(f32) - mean
    scaled = centered * (1.0 + mod_buf[1, :, cols])
    down = iota((ROWS - feats, window), 0)
    tail = jnp.where(down < 2, jnp.broadcast_to(mod_buf[0, :, cols], down.shape), 0.0)
    stacked = jnp.concatenate([scaled, tail], axis=0)
    stacked = pltpu.roll(stacked, (window - (begin - low)) % window, 1)
    a = jnp.concatenate(split(stacked), axis=0)[:, :rows]
    for one in loads[2:]:
        one.wait()
    place = place_ref[2]
    _, sides = layout(local_pairs, width // fold, slots, fold)
    for owner in range(width):
        z, y = divmod(owner, fold)
        pieces = []
        for slot in range(slots):
            spot = z * slots + slot
            if spot < len(sides[y]):
                pair, sub = sides[y][spot]
                both = dot(a, w_buf[PARTS[sub], :, pair * LANES : (pair + 1) * LANES])
                pieces.append(both[:ROWS] + both[ROWS:])
            else:
                pieces.append(jnp.zeros((ROWS, LANES), f32))
        value = jnp.concatenate(pieces, axis=1)
        if direct:
            all_buf[owner ^ place] = value
        else:
            out_refs[0][owner] = value.astype(bf16)
    if direct:
        for d, ref in enumerate(out_refs):
            ref[...] = all_buf[d].astype(ref.dtype)


def sum_kernel(parts_ref, out_ref, *, width):
    total = parts_ref[0].astype(f32)
    for i in range(1, width):
        total = total + parts_ref[i].astype(f32)
    out_ref[...] = total.astype(bf16)


def direct_sum_kernel(*refs):
    *parts, out_ref = refs
    total = parts[0][...]
    for ref in parts[1:]:
        total = total + ref[...].astype(f32)
    out_ref[...] = total.astype(bf16)


def window_kernel(
    place_ref, start_ref, own_ref, right_ref, further_ref, wp_ref,
    x_ref, xt_ref, var_ref, varrow_ref, hid_ref,
    rows_buf, xt_buf, w_ref, own_buf, sem,
):
    load = pltpu.make_async_copy(wp_ref, w_ref, sem.at[0])
    load_own = pltpu.make_async_copy(own_ref, own_buf, sem.at[1])
    load_own.start()
    load.start()
    channels, height, columns = own_ref.shape
    offset = start_ref[...] - place_ref[2] * columns
    for r in range(height):
        at = slice(r * channels, (r + 1) * channels)
        rows_buf[at, columns : 2 * columns] = right_ref[:, r, :].astype(bf16)
        rows_buf[at, 2 * columns :] = further_ref[:, r, :].astype(bf16)
    load_own.wait()
    for r in range(height):
        at = slice(r * channels, (r + 1) * channels)
        rows_buf[at, :columns] = own_buf[:, r, :].astype(bf16)
    col = iota((3 * columns, 2 * columns), 0)
    spot = iota((3 * columns, 2 * columns), 1)
    b = (spot >= columns).astype(jnp.int32)
    pick = jnp.where(col == offset + 2 * (spot - b * columns) + b, 1.0, 0.0).astype(bf16)
    placed = dot(rows_buf[...], pick).astype(bf16)
    tokens = height // 2 * columns
    for p in range(height // 2):
        for a in range(2):
            for b in range(2):
                f = (a * 2 + b) * channels
                xt_buf[f : f + channels, p * columns : (p + 1) * columns] = placed[
                    (2 * p + a) * channels : (2 * p + a + 1) * channels, b * columns : (b + 1) * columns
                ].astype(f32)
    feats = 4 * channels
    xt = xt_buf[:feats, :]
    xpad = jnp.concatenate([xt, jnp.zeros((LANES - feats, tokens), f32)], axis=0)
    xrow = xpad.T
    model = w_ref.shape[1]
    block = 64
    x_bf = xrow[:, :feats].astype(bf16)
    load.wait()
    hid_ref[...] = dot(x_bf, w_ref[...])

    def stats(i, carry):
        at = pl.ds(pl.multiple_of(i * block, block), block)
        h = hid_ref[at, :]
        mean = jnp.sum(h, axis=1, keepdims=True) * (1.0 / model)
        c = h - mean
        v = jnp.sum(c * c, axis=1, keepdims=True) * (1.0 / model)
        var_ref[at, :] = jnp.broadcast_to(v, (block, LANES))
        return carry

    lax.fori_loop(0, tokens // block, stats, 0)
    var = var_ref[...]
    std_hi, std_lo = split(jnp.sqrt(var + epsilon))
    spots = iota((tokens, LANES), 1)
    x_ref[...] = jnp.where(
        spots == feats, std_hi.astype(f32), jnp.where(spots == feats + 1, std_lo.astype(f32), xrow)
    ).astype(bf16)
    var_t = var.T[:8]
    varrow_ref[...] = var_t
    hi_t, lo_t = split(jnp.sqrt(var_t + epsilon))
    down = iota((8, tokens), 0)
    tail = jnp.where(down == 0, hi_t.astype(f32), jnp.where(down == 1, lo_t.astype(f32), 0.0))
    xt_ref[...] = jnp.concatenate([xt, tail], axis=0).astype(bf16)


def attend_units(place_ref, near_ref, far_ref, x_ref, xt_ref, var_ref, varrow_ref, put, units, slots, pairs, fold):
    tokens = x_ref.shape[0]
    key = place_ref[3]
    side = place_ref[2] % fold
    whole, sides = layout(pairs, near_ref.shape[0], slots, fold)
    x = x_ref[:, :ROWS]
    scale = LOG2E * HEAD**-0.5

    xt = xt_ref[...]
    var = var_ref[...]
    rstd = lax.rsqrt(var + epsilon)
    eps_col = epsilon * (var + epsilon)
    eps_row = epsilon * (varrow_ref[:1, :] + epsilon)
    low = iota((tokens, LANES), 1) < HEAD
    ones = jnp.where(low, 1.0, 0.0).astype(bf16)
    other = jnp.where(low, 0.0, 1.0).astype(bf16)
    blank = jnp.zeros((HEAD, tokens), bf16)

    def read(ref, spot):
        slot = spot % slots
        return ref[(spot // slots) ^ key, :, slot * LANES : (slot + 1) * LANES]

    def tile(unit, sub):
        if unit < whole:
            return read(near_ref, 3 * unit + sub)
        if unit < fold * whole:
            return read(far_ref, 3 * (unit - whole) + sub)
        y = next(y for y in range(fold) if (unit, sub) in sides[y])
        spot = sides[y].index((unit, sub))
        return jnp.where(side == y, read(near_ref, spot), read(far_ref, spot))

    for unit in range(*units):
        mq, mv, mk = (tile(unit, sub) for sub in range(3))
        both = dot(x, jnp.concatenate([mq, mv], axis=1))
        uq = both[:, :LANES]
        uv = both[:, LANES:] * rstd
        uk = dot(mk, xt, ((0,), (0,)))
        sq = uq * uq
        sum_low = jnp.sum(jnp.where(low, sq, 0.0), axis=1, keepdims=True)
        sum_high = jnp.sum(jnp.where(low, 0.0, sq), axis=1, keepdims=True)
        q = (uq * lax.rsqrt(jnp.where(low, sum_low, sum_high) * (1.0 / HEAD) + eps_col)).astype(bf16)
        weights = []
        for half in range(2):
            k = uk[half * HEAD : (half + 1) * HEAD]
            mean = jnp.sum(k * k, axis=0, keepdims=True) * (1.0 / HEAD)
            k = (k * lax.rsqrt(mean + eps_row)).astype(bf16)
            kt = jnp.concatenate([k, blank] if half == 0 else [blank, k], axis=0)
            weights.append(jnp.exp2(dot(q, kt) * scale).astype(bf16))
        values = jnp.concatenate(
            [
                jnp.concatenate([jnp.where(low, uv, 0.0).astype(bf16), ones], axis=1),
                jnp.concatenate([jnp.where(low, 0.0, uv).astype(bf16), other], axis=1),
            ],
            axis=0,
        )
        mixed = dot(jnp.concatenate(weights, axis=1), values)
        put(unit, (mixed[:, :LANES] / mixed[:, LANES:]).astype(bf16))


def attend_kernel(
    place_ref, near_ref, far_ref, x_ref, xt_ref, var_ref, varrow_ref, att_ref, *, units, slots, pairs, fold
):
    def put(unit, value):
        at = (unit - units[0]) * LANES
        att_ref[:, at : at + LANES] = value

    attend_units(
        place_ref, near_ref, far_ref, x_ref, xt_ref, var_ref, varrow_ref, put, units, slots, pairs, fold
    )


def near_kernel(place_ref, near_ref, x_ref, xt_ref, var_ref, varrow_ref, att_ref, **sizes):
    attend_kernel(place_ref, near_ref, near_ref, x_ref, xt_ref, var_ref, varrow_ref, att_ref, **sizes)


def second_kernel(
    place_ref, near_ref, far_ref, x_ref, xt_ref, var_ref, varrow_ref, hid_ref, mod_ref, wf_ref, wo_ref, *refs,
    slots, pairs, channels, height, columns, halves, fold, whole,
):
    *att_refs, mine_ref, send_ref, att_buf, res_buf, fin_buf, sum_buf = refs
    group = place_ref[0]
    guide = place_ref[1]
    side = place_ref[2] % fold

    def lanes(half, unit):
        far = jnp.logical_and(unit >= whole, unit < fold * whole)
        at = jnp.where(far, unit - whole + (1 - side) * whole, unit + side * whole)
        at = jnp.where(unit >= fold * whole, unit, at) + half * pairs
        return pl.ds(pl.multiple_of(at * LANES, LANES), LANES)

    unit = 0
    for ref in att_refs:
        for at in range(0, ref.shape[1], LANES):
            att_buf[:, lanes(group, unit)] = ref[:, at : at + LANES]
            unit += 1
    if halves == 2:

        def put(unit, value):
            att_buf[:, lanes(1 - group, unit)] = value

        attend_units(
            place_ref, near_ref, far_ref, x_ref, xt_ref, var_ref, varrow_ref, put, (0, pairs), slots, pairs, fold
        )
    _, model = hid_ref.shape
    sum_buf[...] = jnp.zeros(sum_buf.shape, f32)

    def folded(value):
        total = value[:, :LANES]
        for at in range(LANES, value.shape[1], LANES):
            total = total + value[:, at : at + LANES]
        return total

    def project(cols):
        mixed = dot(att_buf[...], wo_ref[:, cols])
        value = hid_ref[:, cols] + mod_ref[2, :, cols] * mixed
        res_buf[:, cols] = value
        sum_buf[...] = sum_buf[...] + folded(value)

    def sweep(step):
        for at in range(0, model, 2 * LANES):
            step(slice(at, min(at + 2 * LANES, model)))

    sweep(project)
    mean = jnp.sum(sum_buf[...], axis=1, keepdims=True) * (1.0 / model)
    sum_buf[...] = jnp.zeros(sum_buf.shape, f32)

    def center(cols):
        value = res_buf[:, cols] - mean
        fin_buf[:, cols] = value.astype(bf16)
        sum_buf[...] = sum_buf[...] + folded(value * value)

    sweep(center)
    spread = jnp.sum(sum_buf[...], axis=1, keepdims=True) * (1.0 / model)
    result = dot(fin_buf[...], wf_ref[...], ((1,), (1,))) * lax.rsqrt(spread + epsilon)
    near = height // 2 + 1
    keep = guide * (near - 2)
    give = (1 - guide) * (near - 2)
    for p in range(height // 2):
        turned = result[p * columns : (p + 1) * columns].T
        for a in range(2):
            r = 2 * p + a
            for b in range(2):
                f = (a * 2 + b) * channels
                piece = turned[f : f + channels]

                @pl.when(jnp.logical_and(r >= keep, r < keep + near))
                def _():
                    mine_ref[r - keep, :, b * columns : (b + 1) * columns] = piece

                @pl.when(jnp.logical_and(r >= give, r < give + near))
                def _():
                    send_ref[r - give, :, b * columns : (b + 1) * columns] = piece.astype(bf16)


def spread_kernel(
    place_ref, start_ref, mine_ref, theirs_ref, lat_ref, own_ref, odd_ref, two_ref, even_ref
):
    guide = place_ref[1]
    place = place_ref[2]
    near, channels, wide = mine_ref.shape
    columns = wide // 2
    offset = start_ref[...] - place * columns
    flat = near * channels
    first = guide * (near - 2)
    mine = mine_ref[...].reshape(flat, wide)
    theirs = theirs_ref[...].reshape(flat, wide).astype(f32)
    cond = jnp.where(guide == 0, mine, theirs)
    plain = jnp.where(guide == 0, theirs, mine)
    guided = plain + guidance * (cond - plain)
    high, low = split(guided)
    spot = iota((wide, 2 * columns), 0)
    lane = iota((wide, 2 * columns), 1)
    b = (spot >= columns).astype(jnp.int32)
    col = offset + 2 * (spot - b * columns) + b
    target = jnp.where(lane < columns, lane, jnp.where(lane == columns, -1, lane - 1))
    target = jnp.where(lane > columns + 1, -4 * wide, target)
    edge = iota((flat, columns), 1)

    def spots(distance):
        return jnp.where(col == target + distance * columns, 1.0, 0.0).astype(bf16)

    def flagged(values, distance):
        for at, column in ((2, distance * columns - 1), (3, (distance + 1) * columns)):
            covered = jnp.logical_and(column >= offset, column < offset + wide)
            values = jnp.where(edge == at, jnp.where(covered, 1.0, 0.0), values)
        return values

    latent = jnp.concatenate(
        [lat_ref[:, pl.ds(first + i, 1), :].reshape(channels, columns) for i in range(near)], axis=0
    )
    top = latent.astype(bf16).astype(f32)
    middle = (latent - top).astype(bf16).astype(f32)
    bottom = latent - top - middle

    def border(values, column):
        for at, part in enumerate((top, middle, bottom)):
            moved = pltpu.roll(part, (4 + at - column) % columns, 1)
            values = jnp.where(edge == 4 + at, moved, values)
        return values

    here = spots(0)
    own = dot(high, here) + dot(low, here)
    own_ref[:, :columns] = own[:, :columns]
    own_ref[:, columns:] = flagged(own[:, columns:], 0)
    one = dot(high, spots(1))
    one_edge = border(flagged(one[:, columns:], 1), columns - 1)
    two = dot(high, spots(2))
    two_ref[:, :columns] = two[:, :columns].astype(bf16)
    two_ref[:, columns:] = flagged(two[:, columns:], 2).astype(bf16)
    back = dot(high, spots(-1)[:, columns:])
    back_edge = border(flagged(back, -1), 0)
    odd = place % 2 == 1
    odd_ref[:, :columns] = one[:, :columns].astype(bf16)
    even_ref[:, :columns] = one[:, :columns].astype(bf16)
    odd_ref[:, columns:] = jnp.where(odd, one_edge, back_edge).astype(bf16)
    even_ref[:, columns:] = jnp.where(odd, back_edge, one_edge).astype(bf16)


def decode_kernel(
    place_ref, step_ref, own_ref, odd_ref, two_ref, even_ref, lat_ref, count_ref, w_ref, den_ref, feat_out, pad_buf, feat_ref, sems,
    *, width,
):
    guide = place_ref[1]
    place = place_ref[2]
    channels, height, columns = lat_ref.shape
    half = height // 2
    near = half + 1
    flat = near * channels
    first = guide * (near - 2)
    fraction = (jnp.broadcast_to(step_ref[...], (1, columns)).astype(f32) + 1.0) / STEPS
    sigma = 3.0 * fraction / (1.0 + 2.0 * fraction)
    odd = place % 2 == 1
    one = jnp.where(odd, even_ref[...], odd_ref[...]).astype(f32)
    back = jnp.where(odd, odd_ref[:, columns:], even_ref[:, columns:]).astype(f32)
    total = own_ref[...] + one + two_ref[...].astype(f32)
    latent = jnp.concatenate(
        [lat_ref[:, pl.ds(first + i, 1), :].reshape(channels, columns) for i in range(near)], axis=0
    )
    main = latent - sigma * (total[:, :columns] / count_ref[...].astype(f32))
    edges = total[:, columns:] + back
    left = one[:, columns + 4 : columns + 5] + one[:, columns + 5 : columns + 6] + one[:, columns + 6 : columns + 7]
    right = back[:, 4:5] + back[:, 5:6] + back[:, 6:7]
    left = left - sigma[:, :1] * (edges[:, 0:1] / edges[:, 2:3])
    right = right - sigma[:, :1] * (edges[:, 1:2] / edges[:, 3:4])
    left = jnp.where(place == 0, 0.0, left)
    right = jnp.where(place == width - 1, 0.0, right)
    lane = iota((flat, columns), 1)
    before = jnp.where(lane == 0, left, pltpu.roll(main, 1, 1))
    after = jnp.where(lane == columns - 1, right, pltpu.roll(main, columns - 1, 1))
    zero = jnp.zeros((channels, columns), f32)
    for b, value in enumerate((before, main, after)):
        pad_buf[b, 0] = zero
        pad_buf[b, near + 1] = zero
        for i in range(near):
            pad_buf[b, i + 1] = value[i * channels : (i + 1) * channels]
    saves = []
    for r in range(half):
        at = guide + r
        den_ref[:, r, :] = pad_buf[1, at + 1]
        stacked = jnp.concatenate(
            [pad_buf[b, at + a] for a in range(3) for b in range(3)], axis=0
        ).astype(bf16)
        summed = dot(stacked, w_ref[...], ((0,), (0,)))
        feat_ref[r] = (summed / (1.0 + jnp.exp(-summed))).astype(bf16)
        saves.append(pltpu.make_async_copy(feat_ref.at[r], feat_out.at[r], sems.at[r]))
        saves[-1].start()
    for one in saves:
        one.wait()


def shift(x, by):
    peers = lax.axis_size("width")
    return lax.ppermute(x, "width", [(i, (i + by) % peers) for i in range(peers)])


def swap(x, axis):
    return lax.ppermute(x, axis, [(0, 1), (1, 0)])


def send_xor(x, d):
    width = lax.axis_size("width")
    return lax.ppermute(x, "width", [(i, i ^ d) for i in range(width)])


def gather_major(chunk, fold, direct):
    width = lax.axis_size("width")
    depth = width // fold
    if not direct:
        every = lax.all_gather(chunk, "width")
        every = every.reshape((depth, fold) + chunk.shape)
        return lax.dynamic_index_in_dim(every, lax.axis_index("width") % fold, 1, False)
    got = [send_xor(chunk, d * fold) for d in range(depth - 1, 0, -1)]
    return jnp.stack([chunk] + got[::-1])


def swap_minor(stack):
    width = lax.axis_size("width")
    return lax.ppermute(stack, "width", [(i, i ^ 1) for i in range(width)])


def shards(latent, starts, counts, step_index, cond_mod, w_patch, w_qkv, w_out, w_final, w_dec):
    guide = lax.axis_index("guide")
    place = lax.axis_index("width")
    group = lax.axis_index("groups")
    width = lax.axis_size("width")
    channels, height, columns = latent.shape
    model = w_patch.shape[1]
    feats = w_patch.shape[0]
    features = HEADS * HEAD
    pairs = features // LANES
    halves = 2 if lax.axis_size("groups") == 2 and pairs % 2 == 0 else 1
    local_pairs = pairs // halves
    slots = -(-3 * local_pairs // width)
    if halves == 1:
        group = group * 0
    rows = w_qkv.shape[0]
    fold = 2
    direct = width <= 8 and width & (width - 1) == 0
    changes = jnp.swapaxes(cond_mod, 0, 1)
    key = place // fold if direct else 0
    scalars = jnp.stack([group, guide, place, key]).astype(jnp.int32)

    right = shift(latent, -1)
    further = shift(latent, -2)

    slab = (ROWS, slots * LANES)
    in_hbm = functools.partial(pltpu.with_memory_space_constraint, memory_space=pltpu.HBM)
    parts = call(
        functools.partial(
            partial_kernel, width=width, slots=slots, local_pairs=local_pairs, features=features,
            fold=fold, direct=direct,
        ),
        [(slab, f32)] + [(slab, bf16)] * (width - 1) if direct else [((width,) + slab, bf16)],
        scratch=[
            pltpu.VMEM((3, rows, local_pairs * LANES), bf16),
            pltpu.VMEM(changes.shape, f32),
            pltpu.VMEM(w_patch.shape, bf16),
            pltpu.VMEM((width,) + slab if direct else slab, f32),
            pltpu.SemaphoreType.DMA((5,)),
        ],
        anys=(1, 2, 3), smem=(0,), count=4, limit=8,
    )(scalars, in_hbm(changes), in_hbm(w_patch), in_hbm(w_qkv))
    near = height // 2 + 1
    tokens = height // 2 * columns
    if direct:
        came = [send_xor(parts[d], d) for d in range(width - 1, 0, -1)]
    else:
        came = lax.all_to_all(parts[0], "width", 0, 0, tiled=True)
    x, xt, var, varrow, hidden = call(
        window_kernel,
        [
            ((tokens, LANES), bf16), ((ROWS, tokens), bf16), ((tokens, LANES), f32), ((8, tokens), f32),
            ((tokens, model), f32),
        ],
        scratch=[
            pltpu.VMEM((height * channels, 3 * columns), bf16),
            pltpu.VMEM((feats, tokens), f32),
            pltpu.VMEM(w_patch.shape, bf16),
            pltpu.VMEM(latent.shape, f32),
            pltpu.SemaphoreType.DMA((2,)),
        ],
        anys=(2, 5), smem=(0,), count=6, flops=5e9,
    )(scalars, starts[None], in_hbm(latent), right, further, in_hbm(w_patch))
    came, x = lax.optimization_barrier((came, x))
    if direct:
        (chunk,) = call(direct_sum_kernel, [(slab, bf16)], count=width, limit=4)(parts[0], *came)
    else:
        (chunk,) = call(
            functools.partial(sum_kernel, width=width), [(slab, bf16)], count=1, limit=4
        )(came)
    stack = gather_major(chunk, fold, direct)
    side = swap_minor(stack)
    stack_x = swap(stack, "groups") if halves == 2 else stack
    whole = local_pairs // fold
    sizes = dict(slots=slots, pairs=local_pairs, fold=fold)
    (att_near,) = call(
        functools.partial(near_kernel, units=(0, whole), **sizes),
        [((tokens, whole * LANES), bf16)],
        smem=(0,), count=6, flops=2e9,
    )(scalars, stack, x, xt, var, varrow)
    side, att_near = lax.optimization_barrier((side, att_near))
    if halves == 2:
        side_x = swap(side, "groups")
    else:
        side_x = side
    (att_far,) = call(
        functools.partial(attend_kernel, units=(whole, local_pairs), **sizes),
        [((tokens, (local_pairs - whole) * LANES), bf16)],
        smem=(0,), count=7, flops=3e9,
    )(scalars, stack, side, x, xt, var, varrow)
    mine_v, send_v = call(
        functools.partial(
            second_kernel, channels=channels, height=height, columns=columns, halves=halves, whole=whole, **sizes
        ),
        [((near, channels, 2 * columns), f32), ((near, channels, 2 * columns), bf16)],
        scratch=[
            pltpu.VMEM((tokens, features), bf16),
            pltpu.VMEM((tokens, model), f32),
            pltpu.VMEM((tokens, model), bf16),
            pltpu.VMEM((tokens, LANES), f32),
        ],
        smem=(0,), count=13, flops=12e9, limit=22,
    )(scalars, stack_x, side_x, x, xt, var, varrow, hidden, changes, w_final.T, w_out, att_near, att_far)
    theirs = swap(send_v, "guide")
    flat = near * channels
    own, odd, two, even = call(
        spread_kernel,
        [
            ((flat, 2 * columns), f32), ((flat, 2 * columns), bf16),
            ((flat, 2 * columns), bf16), ((flat, 2 * columns), bf16),
        ],
        smem=(0,), count=5, limit=8,
    )(scalars, starts[None], mine_v, theirs, latent)
    ups = [(i, (i + 1) % width) for i in range(width)]
    turns = [[pair for pair in ups if pair[0] % 2 == side] for side in range(2)]
    turns = [pairs + [(b, a) for a, b in pairs] for pairs in turns]
    odd = lax.ppermute(odd, "width", turns[1])
    two = lax.ppermute(two, "width", [(i, (i + 2) % width) for i in range(width)])
    even = lax.ppermute(even, "width", turns[0])
    return call(
        functools.partial(decode_kernel, width=width),
        [((channels, height // 2, columns), f32), ((height // 2, columns, w_dec.shape[1]), bf16)],
        scratch=[
            pltpu.VMEM((3, near + 2, channels, columns), f32),
            pltpu.VMEM((height // 2, columns, w_dec.shape[1]), bf16),
            pltpu.SemaphoreType.DMA((height // 2,)),
        ],
        smem=(0,), count=9, limit=8, hbm_outs=(1,),
    )(scalars, step_index[None], own, odd, two, even, latent, counts[None], w_dec)


def solution(mesh):
    return jax.shard_map(
        shards,
        mesh=mesh,
        in_specs=(
            P(None, None, ("groups", "width")),
            P(("groups", "width")),
            P(("groups", "width")),
            P("groups"),
            P("guide", None, None),
            P(),
            P("width", None),
            P(),
            P(),
            P(),
        ),
        out_specs=(P(None, "guide", ("groups", "width")), P("guide", ("groups", "width"), None)),
        check_vma=False,
    )
```

```python
import functools

import jax
import jax.numpy as jnp
from jax import lax
from jax.experimental import pallas as pl
from jax.experimental.pallas import tpu as pltpu
from jax.sharding import PartitionSpec as P


HEADS = 20
HEAD = 64
STEPS = 28
LANES = 128
ROWS = 72


guidance = 4.0
epsilon = 1e-06

bf16 = jnp.bfloat16
f32 = jnp.float32
PARTS = (0, 2, 1)
LOG2E = 1.4426950408889634


def dot(a, b, dims=((1,), (0,))):
    return lax.dot_general(a, b, (dims, ((), ())), preferred_element_type=f32)


def call(body, outs, scratch=(), anys=(), smem=(), count=0, limit=16, flops=0):
    def spec(i):
        if i in anys:
            return pl.BlockSpec(memory_space=pltpu.HBM)
        if i in smem:
            return pl.BlockSpec(memory_space=pltpu.SMEM)
        return pl.BlockSpec(memory_space=pltpu.VMEM)

    return pl.pallas_call(
        body,
        out_shape=tuple(jax.ShapeDtypeStruct(s, t) for s, t in outs),
        in_specs=[spec(i) for i in range(count)],
        out_specs=tuple(pl.BlockSpec(memory_space=pltpu.VMEM) for _ in outs),
        scratch_shapes=list(scratch),
        compiler_params=pltpu.CompilerParams(vmem_limit_bytes=limit << 20),
        cost_estimate=pl.CostEstimate(flops=int(flops), bytes_accessed=1 << 20, transcendentals=0),
    )


def iota(shape, dim):
    return lax.broadcasted_iota(jnp.int32, shape, dim)


def folded(value):
    total = value[:, :LANES]
    for at in range(LANES, value.shape[1], LANES):
        total = total + value[:, at : at + LANES]
    return total


def layout(local_pairs, depth, slots, fold):
    whole = local_pairs // fold
    sides = [[(y * whole + j, sub) for j in range(whole) for sub in range(3)] for y in range(fold)]
    for pair in range(fold * whole, local_pairs):
        for sub in range(3):
            y = next(y for y in range(fold) if len(sides[y]) < depth * slots)
            sides[y].append((pair, sub))
    return whole, sides


def split(values):
    high = values.astype(bf16)
    return high, (values - high.astype(f32)).astype(bf16)


def partial_kernel(
    place_ref, mod_ref, wp_ref, w_ref, *refs, width, slots, local_pairs, features, fold, direct
):
    *out_refs, w_buf, mod_buf, wp_buf, all_buf, sems = refs
    group = place_ref[0]
    span = local_pairs * LANES
    loads = [
        pltpu.make_async_copy(wp_ref, wp_buf, sems.at[0]),
        pltpu.make_async_copy(mod_ref, mod_buf, sems.at[1]),
    ]
    for part in range(3):
        start = pl.multiple_of(part * features + group * span, LANES)
        loads.append(
            pltpu.make_async_copy(w_ref.at[:, pl.ds(start, span)], w_buf.at[part], sems.at[2 + part])
        )
    for one in loads:
        one.start()
    feats, model = wp_ref.shape
    rows = w_buf.shape[1]
    window = min(model, -(-(rows + LANES - 1) // LANES) * LANES)
    begin = place_ref[2] * rows
    low = jnp.minimum(begin // LANES * LANES, model - window)
    cols = pl.ds(pl.multiple_of(low, LANES), window)
    loads[0].wait()
    loads[1].wait()
    mean = jnp.sum(wp_buf[...].astype(f32), axis=1, keepdims=True) * (1.0 / model)
    centered = wp_buf[:, cols].astype(f32) - mean
    scaled = centered * (1.0 + mod_buf[1, :, cols])
    down = iota((ROWS - feats, window), 0)
    tail = jnp.where(down < 2, jnp.broadcast_to(mod_buf[0, :, cols], down.shape), 0.0)
    stacked = jnp.concatenate([scaled, tail], axis=0)
    stacked = pltpu.roll(stacked, (window - (begin - low)) % window, 1)
    a = jnp.concatenate(split(stacked), axis=0)[:, :rows]
    for one in loads[2:]:
        one.wait()
    place = place_ref[2]
    _, sides = layout(local_pairs, width // fold, slots, fold)
    for owner in range(width):
        z, y = divmod(owner, fold)
        pieces = []
        for slot in range(slots):
            spot = z * slots + slot
            if spot < len(sides[y]):
                pair, sub = sides[y][spot]
                both = dot(a, w_buf[PARTS[sub], :, pair * LANES : (pair + 1) * LANES])
                pieces.append(both[:ROWS] + both[ROWS:])
            else:
                pieces.append(jnp.zeros((ROWS, LANES), f32))
        value = jnp.concatenate(pieces, axis=1)
        if direct:
            all_buf[(place ^ y) % fold, z] = value
        else:
            out_refs[0][owner] = value.astype(bf16)
    if direct:
        for side, ref in enumerate(out_refs):
            ref[...] = all_buf[side].astype(ref.dtype)


def sum_kernel(parts_ref, out_ref, *, width):
    total = parts_ref[0].astype(f32)
    for i in range(1, width):
        total = total + parts_ref[i].astype(f32)
    out_ref[...] = total.astype(bf16)


def first_sum_kernel(place_ref, keep_ref, came_ref, own_ref, *send_refs):
    key = place_ref[3]
    own_ref[...] = keep_ref[key] + came_ref[key].astype(f32)
    for d, ref in enumerate(send_refs):
        at = key ^ (d + 1)
        ref[...] = (keep_ref[at] + came_ref[at].astype(f32)).astype(bf16)


def last_sum_kernel(*refs):
    *parts, out_ref = refs
    total = parts[0][...]
    for ref in parts[1:]:
        total = total + ref[...].astype(f32)
    out_ref[...] = total.astype(bf16)


def window_kernel(
    place_ref, start_ref, own_ref, right_ref, further_ref, wp_ref,
    x_ref, xt_ref, var_ref, varrow_ref, hid_ref, facts_ref,
    rows_buf, xt_buf, sum_buf, w_ref, own_buf, sem,
):
    load = pltpu.make_async_copy(wp_ref, w_ref, sem.at[0])
    load_own = pltpu.make_async_copy(own_ref, own_buf, sem.at[1])
    load_own.start()
    load.start()
    channels, height, columns = own_ref.shape
    for r in range(height):
        at = slice(r * channels, (r + 1) * channels)
        rows_buf[at, columns : 2 * columns] = right_ref[:, r, :].astype(bf16)
        rows_buf[at, 2 * columns :] = further_ref[:, r, :].astype(bf16)
    offset = start_ref[0] - place_ref[2] * columns
    facts_ref[...] = jnp.zeros(facts_ref.shape, jnp.int32) + offset
    load_own.wait()
    for r in range(height):
        at = slice(r * channels, (r + 1) * channels)
        rows_buf[at, :columns] = own_buf[:, r, :].astype(bf16)
    col = iota((3 * columns, 2 * columns), 0)
    spot = iota((3 * columns, 2 * columns), 1)
    b = (spot >= columns).astype(jnp.int32)
    pick = jnp.where(col == offset + 2 * (spot - b * columns) + b, 1.0, 0.0).astype(bf16)
    placed = dot(rows_buf[...], pick).astype(bf16)
    tokens = height // 2 * columns
    for p in range(height // 2):
        for a in range(2):
            for b in range(2):
                f = (a * 2 + b) * channels
                xt_buf[f : f + channels, p * columns : (p + 1) * columns] = placed[
                    (2 * p + a) * channels : (2 * p + a + 1) * channels, b * columns : (b + 1) * columns
                ].astype(f32)
    feats = 4 * channels
    xt = xt_buf[:feats, :]
    xpad = jnp.concatenate([xt, jnp.zeros((LANES - feats, tokens), f32)], axis=0)
    xrow = xpad.T
    model = w_ref.shape[1]
    x_bf = xrow[:, :feats].astype(bf16)
    load.wait()
    tiles = [slice(at, min(at + 2 * LANES, model)) for at in range(0, model, 2 * LANES)]
    sum_buf[...] = jnp.zeros(sum_buf.shape, f32)
    for cols in tiles:
        value = dot(x_bf, w_ref[:, cols])
        hid_ref[:, cols] = value
        sum_buf[...] = sum_buf[...] + folded(value)
    mean = jnp.sum(sum_buf[...], axis=1, keepdims=True) * (1.0 / model)
    sum_buf[...] = jnp.zeros(sum_buf.shape, f32)
    for cols in tiles:
        value = hid_ref[:, cols] - mean
        sum_buf[...] = sum_buf[...] + folded(value * value)
    spread = jnp.sum(sum_buf[...], axis=1, keepdims=True) * (1.0 / model)
    var_ref[...] = jnp.broadcast_to(spread, var_ref.shape)
    var = var_ref[...]
    std_hi, std_lo = split(jnp.sqrt(var + epsilon))
    spots = iota((tokens, LANES), 1)
    x_ref[...] = jnp.where(
        spots == feats, std_hi.astype(f32), jnp.where(spots == feats + 1, std_lo.astype(f32), xrow)
    ).astype(bf16)
    var_t = var.T[:8]
    varrow_ref[...] = var_t
    hi_t, lo_t = split(jnp.sqrt(var_t + epsilon))
    down = iota((8, tokens), 0)
    tail = jnp.where(down == 0, hi_t.astype(f32), jnp.where(down == 1, lo_t.astype(f32), 0.0))
    xt_ref[...] = jnp.concatenate([xt, tail], axis=0).astype(bf16)


def attend_units(place_ref, near_ref, far_ref, x_ref, xt_ref, var_ref, varrow_ref, put, units, slots, pairs, fold):
    tokens = x_ref.shape[0]
    key = place_ref[3]
    side = place_ref[2] % fold
    whole, sides = layout(pairs, near_ref.shape[0], slots, fold)
    x = x_ref[:, :ROWS]
    scale = LOG2E * HEAD**-0.5

    xt = xt_ref[...]
    var = var_ref[...]
    rstd = lax.rsqrt(var + epsilon)
    eps_col = epsilon * (var + epsilon)
    eps_row = epsilon * (varrow_ref[:1, :] + epsilon)
    low = iota((tokens, LANES), 1) < HEAD
    ones = jnp.where(low, 1.0, 0.0).astype(bf16)
    other = jnp.where(low, 0.0, 1.0).astype(bf16)
    blank = jnp.zeros((HEAD, tokens), bf16)

    def read(ref, spot):
        slot = spot % slots
        return ref[(spot // slots) ^ key, :, slot * LANES : (slot + 1) * LANES]

    def tile(unit, sub):
        if unit < whole:
            return read(near_ref, 3 * unit + sub)
        if unit < fold * whole:
            return read(far_ref, 3 * (unit - whole) + sub)
        y = next(y for y in range(fold) if (unit, sub) in sides[y])
        spot = sides[y].index((unit, sub))
        return jnp.where(side == y, read(near_ref, spot), read(far_ref, spot))

    for unit in range(*units):
        mq, mv, mk = (tile(unit, sub) for sub in range(3))
        both = dot(x, jnp.concatenate([mq, mv], axis=1))
        uq = both[:, :LANES]
        uv = both[:, LANES:] * rstd
        uk = dot(mk, xt, ((0,), (0,)))
        sq = uq * uq
        sum_low = jnp.sum(jnp.where(low, sq, 0.0), axis=1, keepdims=True)
        sum_high = jnp.sum(jnp.where(low, 0.0, sq), axis=1, keepdims=True)
        q = (uq * lax.rsqrt(jnp.where(low, sum_low, sum_high) * (1.0 / HEAD) + eps_col)).astype(bf16)
        weights = []
        for half in range(2):
            k = uk[half * HEAD : (half + 1) * HEAD]
            mean = jnp.sum(k * k, axis=0, keepdims=True) * (1.0 / HEAD)
            k = (k * lax.rsqrt(mean + eps_row)).astype(bf16)
            kt = jnp.concatenate([k, blank] if half == 0 else [blank, k], axis=0)
            weights.append(jnp.exp2(dot(q, kt) * scale).astype(bf16))
        values = jnp.concatenate(
            [
                jnp.concatenate([jnp.where(low, uv, 0.0).astype(bf16), ones], axis=1),
                jnp.concatenate([jnp.where(low, 0.0, uv).astype(bf16), other], axis=1),
            ],
            axis=0,
        )
        mixed = dot(jnp.concatenate(weights, axis=1), values)
        put(unit, (mixed[:, :LANES] / mixed[:, LANES:]).astype(bf16))


def attend_kernel(
    place_ref, near_ref, far_ref, x_ref, xt_ref, var_ref, varrow_ref, att_ref, *, units, slots, pairs, fold
):
    def put(unit, value):
        at = (unit - units[0]) * LANES
        att_ref[:, at : at + LANES] = value

    attend_units(
        place_ref, near_ref, far_ref, x_ref, xt_ref, var_ref, varrow_ref, put, units, slots, pairs, fold
    )


def near_kernel(place_ref, near_ref, x_ref, xt_ref, var_ref, varrow_ref, att_ref, **sizes):
    attend_kernel(place_ref, near_ref, near_ref, x_ref, xt_ref, var_ref, varrow_ref, att_ref, **sizes)


def second_kernel(
    place_ref, near_ref, far_ref, x_ref, xt_ref, var_ref, varrow_ref, hid_ref, mod_ref, wf_ref, wo_ref, *refs,
    slots, pairs, channels, height, columns, halves, fold, whole,
):
    *att_refs, mine_ref, send_ref, att_buf, res_buf, fin_buf, sum_buf = refs
    group = place_ref[0]
    guide = place_ref[1]
    side = place_ref[2] % fold

    def lanes(half, unit):
        far = jnp.logical_and(unit >= whole, unit < fold * whole)
        at = jnp.where(far, unit - whole + (1 - side) * whole, unit + side * whole)
        at = jnp.where(unit >= fold * whole, unit, at) + half * pairs
        return pl.ds(pl.multiple_of(at * LANES, LANES), LANES)

    unit = 0
    for ref in att_refs:
        for at in range(0, ref.shape[1], LANES):
            att_buf[:, lanes(group, unit)] = ref[:, at : at + LANES]
            unit += 1
    if halves == 2:

        def put(unit, value):
            att_buf[:, lanes(1 - group, unit)] = value

        attend_units(
            place_ref, near_ref, far_ref, x_ref, xt_ref, var_ref, varrow_ref, put, (0, pairs), slots, pairs, fold
        )
    _, model = hid_ref.shape
    sum_buf[...] = jnp.zeros(sum_buf.shape, f32)

    def project(cols):
        mixed = dot(att_buf[...], wo_ref[:, cols])
        value = hid_ref[:, cols] + mod_ref[2, :, cols] * mixed
        res_buf[:, cols] = value
        sum_buf[...] = sum_buf[...] + folded(value)

    def sweep(step):
        for at in range(0, model, 2 * LANES):
            step(slice(at, min(at + 2 * LANES, model)))

    sweep(project)
    mean = jnp.sum(sum_buf[...], axis=1, keepdims=True) * (1.0 / model)
    sum_buf[...] = jnp.zeros(sum_buf.shape, f32)

    def center(cols):
        value = res_buf[:, cols] - mean
        fin_buf[:, cols] = value.astype(bf16)
        sum_buf[...] = sum_buf[...] + folded(value * value)

    sweep(center)
    spread = jnp.sum(sum_buf[...], axis=1, keepdims=True) * (1.0 / model)
    result = dot(fin_buf[...], wf_ref[...], ((1,), (1,))) * lax.rsqrt(spread + epsilon)
    near = height // 2 + 1
    keep = guide * (near - 2)
    give = (1 - guide) * (near - 2)
    for p in range(height // 2):
        turned = result[p * columns : (p + 1) * columns].T
        for a in range(2):
            r = 2 * p + a
            for b in range(2):
                f = (a * 2 + b) * channels
                piece = turned[f : f + channels]

                @pl.when(jnp.logical_and(r >= keep, r < keep + near))
                def _():
                    mine_ref[r - keep, :, b * columns : (b + 1) * columns] = piece

                @pl.when(jnp.logical_and(r >= give, r < give + near))
                def _():
                    send_ref[r - give, :, b * columns : (b + 1) * columns] = piece.astype(bf16)


def spread_kernel(
    place_ref, facts_ref, mine_ref, theirs_ref, lat_ref, own_ref, odd_ref, two_ref, even_ref
):
    guide = place_ref[1]
    place = place_ref[2]
    near, channels, wide = mine_ref.shape
    columns = wide // 2
    offset = facts_ref[0:1, 0:1]
    flat = near * channels
    first = guide * (near - 2)
    mine = mine_ref[...].reshape(flat, wide)
    theirs = theirs_ref[...].reshape(flat, wide).astype(f32)
    cond = jnp.where(guide == 0, mine, theirs)
    plain = jnp.where(guide == 0, theirs, mine)
    guided = plain + guidance * (cond - plain)
    high, low = split(guided)
    spot = iota((wide, 2 * columns), 0)
    lane = iota((wide, 2 * columns), 1)
    b = (spot >= columns).astype(jnp.int32)
    col = offset + 2 * (spot - b * columns) + b
    target = jnp.where(lane < columns, lane, jnp.where(lane == columns, -1, lane - 1))
    target = jnp.where(lane > columns + 1, -4 * wide, target)
    edge = iota((flat, columns), 1)

    def spots(distance):
        return jnp.where(col == target + distance * columns, 1.0, 0.0).astype(bf16)

    def flagged(values, distance):
        for at, column in ((2, distance * columns - 1), (3, (distance + 1) * columns)):
            covered = jnp.logical_and(column >= offset, column < offset + wide)
            values = jnp.where(edge == at, jnp.where(covered, 1.0, 0.0), values)
        return values

    latent = jnp.concatenate(
        [lat_ref[:, pl.ds(first + i, 1), :].reshape(channels, columns) for i in range(near)], axis=0
    )
    top = latent.astype(bf16).astype(f32)
    middle = (latent - top).astype(bf16).astype(f32)
    bottom = latent - top - middle

    def border(values, column):
        for at, part in enumerate((top, middle, bottom)):
            moved = pltpu.roll(part, (4 + at - column) % columns, 1)
            values = jnp.where(edge == 4 + at, moved, values)
        return values

    here = spots(0)
    own = dot(high, here) + dot(low, here)
    own_ref[:, :columns] = own[:, :columns]
    own_ref[:, columns:] = flagged(own[:, columns:], 0)
    one = dot(high, spots(1))
    one_edge = border(flagged(one[:, columns:], 1), columns - 1)
    two = dot(high, spots(2))
    two_ref[:, :columns] = two[:, :columns].astype(bf16)
    two_ref[:, columns:] = flagged(two[:, columns:], 2).astype(bf16)
    back = dot(high, spots(-1)[:, columns:])
    back_edge = border(flagged(back, -1), 0)
    odd = place % 2 == 1
    odd_ref[:, :columns] = one[:, :columns].astype(bf16)
    even_ref[:, :columns] = one[:, :columns].astype(bf16)
    odd_ref[:, columns:] = jnp.where(odd, one_edge, back_edge).astype(bf16)
    even_ref[:, columns:] = jnp.where(odd, back_edge, one_edge).astype(bf16)


def decode_kernel(
    place_ref, step_ref, own_ref, odd_ref, two_ref, even_ref, lat_ref, count_ref, w_ref, den_ref, feat_ref, pad_buf,
    *, width,
):
    guide = place_ref[1]
    place = place_ref[2]
    channels, height, columns = lat_ref.shape
    half = height // 2
    near = half + 1
    flat = near * channels
    first = guide * (near - 2)
    fraction = (jnp.full((1, columns), step_ref[0], jnp.int32).astype(f32) + 1.0) / STEPS
    sigma = 3.0 * fraction / (1.0 + 2.0 * fraction)
    odd = place % 2 == 1
    one = jnp.where(odd, even_ref[...], odd_ref[...]).astype(f32)
    back = jnp.where(odd, odd_ref[:, columns:], even_ref[:, columns:]).astype(f32)
    total = own_ref[...] + one + two_ref[...].astype(f32)
    latent = jnp.concatenate(
        [lat_ref[:, pl.ds(first + i, 1), :].reshape(channels, columns) for i in range(near)], axis=0
    )
    main = latent - sigma * (total[:, :columns] / count_ref[...].astype(f32))
    edges = total[:, columns:] + back
    left = one[:, columns + 4 : columns + 5] + one[:, columns + 5 : columns + 6] + one[:, columns + 6 : columns + 7]
    right = back[:, 4:5] + back[:, 5:6] + back[:, 6:7]
    left = left - sigma[:, :1] * (edges[:, 0:1] / edges[:, 2:3])
    right = right - sigma[:, :1] * (edges[:, 1:2] / edges[:, 3:4])
    left = jnp.where(place == 0, 0.0, left)
    right = jnp.where(place == width - 1, 0.0, right)
    lane = iota((flat, columns), 1)
    before = jnp.where(lane == 0, left, pltpu.roll(main, 1, 1))
    after = jnp.where(lane == columns - 1, right, pltpu.roll(main, columns - 1, 1))
    zero = jnp.zeros((channels, columns), f32)
    for b, value in enumerate((before, main, after)):
        pad_buf[b, 0] = zero
        pad_buf[b, near + 1] = zero
        for i in range(near):
            pad_buf[b, i + 1] = value[i * channels : (i + 1) * channels]
    for r in range(half):
        at = guide + r
        den_ref[:, r, :] = pad_buf[1, at + 1]
        stacked = jnp.concatenate(
            [pad_buf[b, at + a] for a in range(3) for b in range(3)], axis=0
        ).astype(bf16)
        summed = dot(stacked, w_ref[...], ((0,), (0,)))
        feat_ref[r] = (summed / (1.0 + jnp.exp(-summed))).astype(bf16)


def shift(x, by):
    peers = lax.axis_size("width")
    return lax.ppermute(x, "width", [(i, (i + by) % peers) for i in range(peers)])


def swap(x, axis):
    return lax.ppermute(x, axis, [(0, 1), (1, 0)])


def send_xor(x, d):
    width = lax.axis_size("width")
    return lax.ppermute(x, "width", [(i, i ^ d) for i in range(width)])


def gather_major(chunk, fold, direct):
    width = lax.axis_size("width")
    depth = width // fold
    if not direct:
        every = lax.all_gather(chunk, "width")
        every = every.reshape((depth, fold) + chunk.shape)
        return lax.dynamic_index_in_dim(every, lax.axis_index("width") % fold, 1, False)
    got = [send_xor(chunk, d * fold) for d in range(depth - 1, 0, -1)]
    return jnp.stack([chunk] + got[::-1])


def swap_minor(stack):
    width = lax.axis_size("width")
    return lax.ppermute(stack, "width", [(i, i ^ 1) for i in range(width)])


def shards(latent, starts, counts, step_index, cond_mod, w_patch, w_qkv, w_out, w_final, w_dec):
    guide = lax.axis_index("guide")
    place = lax.axis_index("width")
    group = lax.axis_index("groups")
    width = lax.axis_size("width")
    channels, height, columns = latent.shape
    model = w_patch.shape[1]
    feats = w_patch.shape[0]
    features = HEADS * HEAD
    pairs = features // LANES
    halves = 2 if lax.axis_size("groups") == 2 and pairs % 2 == 0 else 1
    local_pairs = pairs // halves
    slots = -(-3 * local_pairs // width)
    if halves == 1:
        group = group * 0
    rows = w_qkv.shape[0]
    fold = 2
    depth = width // fold
    direct = width <= 8 and width & (width - 1) == 0
    changes = jnp.swapaxes(cond_mod, 0, 1)
    key = place // fold if direct else 0
    scalars = jnp.stack([group, guide, place, key]).astype(jnp.int32)

    right = shift(latent, -1)
    further = shift(latent, -2)

    slab = (ROWS, slots * LANES)
    in_hbm = functools.partial(pltpu.with_memory_space_constraint, memory_space=pltpu.HBM)
    parts = call(
        functools.partial(
            partial_kernel, width=width, slots=slots, local_pairs=local_pairs, features=features,
            fold=fold, direct=direct,
        ),
        [((depth,) + slab, f32), ((depth,) + slab, bf16)] if direct else [((width,) + slab, bf16)],
        scratch=[
            pltpu.VMEM((3, rows, local_pairs * LANES), bf16),
            pltpu.VMEM(changes.shape, f32),
            pltpu.VMEM(w_patch.shape, bf16),
            pltpu.VMEM((fold, depth) + slab if direct else slab, f32),
            pltpu.SemaphoreType.DMA((5,)),
        ],
        anys=(1, 2, 3), smem=(0,), count=4, limit=8,
    )(scalars, in_hbm(changes), in_hbm(w_patch), in_hbm(w_qkv))
    near = height // 2 + 1
    tokens = height // 2 * columns
    if direct:
        came = send_xor(parts[1], 1)
    else:
        came = lax.all_to_all(parts[0], "width", 0, 0, tiled=True)
    x, xt, var, varrow, hidden, facts = call(
        window_kernel,
        [
            ((tokens, LANES), bf16), ((ROWS, tokens), bf16), ((tokens, LANES), f32), ((8, tokens), f32),
            ((tokens, model), f32), ((8, LANES), jnp.int32),
        ],
        scratch=[
            pltpu.VMEM((height * channels, 3 * columns), bf16),
            pltpu.VMEM((feats, tokens), f32),
            pltpu.VMEM((tokens, LANES), f32),
            pltpu.VMEM(w_patch.shape, bf16),
            pltpu.VMEM(latent.shape, f32),
            pltpu.SemaphoreType.DMA((2,)),
        ],
        anys=(2, 5), smem=(0, 1), count=6, flops=5e9,
    )(scalars, starts, in_hbm(latent), right, further, in_hbm(w_patch))
    came, x = lax.optimization_barrier((came, x))
    if direct:
        own, *sends = call(
            first_sum_kernel, [(slab, f32)] + [(slab, bf16)] * (depth - 1), smem=(0,), count=3, limit=4
        )(scalars, parts[0], came)
        got = [send_xor(sends[d - 1], d * fold) for d in range(depth - 1, 0, -1)]
        (chunk,) = call(last_sum_kernel, [(slab, bf16)], count=depth, limit=4)(own, *got)
    else:
        (chunk,) = call(
            functools.partial(sum_kernel, width=width), [(slab, bf16)], count=1, limit=4
        )(came)
    stack = gather_major(chunk, fold, direct)
    side = swap_minor(stack)
    stack_x = swap(stack, "groups") if halves == 2 else stack
    whole = local_pairs // fold
    sizes = dict(slots=slots, pairs=local_pairs, fold=fold)
    (att_near,) = call(
        functools.partial(near_kernel, units=(0, whole), **sizes),
        [((tokens, whole * LANES), bf16)],
        smem=(0,), count=6, flops=2e9,
    )(scalars, stack, x, xt, var, varrow)
    side, att_near = lax.optimization_barrier((side, att_near))
    if halves == 2:
        side_x = swap(side, "groups")
    else:
        side_x = side
    (att_far,) = call(
        functools.partial(attend_kernel, units=(whole, local_pairs), **sizes),
        [((tokens, (local_pairs - whole) * LANES), bf16)],
        smem=(0,), count=7, flops=3e9,
    )(scalars, stack, side, x, xt, var, varrow)
    mine_v, send_v = call(
        functools.partial(
            second_kernel, channels=channels, height=height, columns=columns, halves=halves, whole=whole, **sizes
        ),
        [((near, channels, 2 * columns), f32), ((near, channels, 2 * columns), bf16)],
        scratch=[
            pltpu.VMEM((tokens, features), bf16),
            pltpu.VMEM((tokens, model), f32),
            pltpu.VMEM((tokens, model), bf16),
            pltpu.VMEM((tokens, LANES), f32),
        ],
        smem=(0,), count=13, flops=12e9, limit=22,
    )(scalars, stack_x, side_x, x, xt, var, varrow, hidden, changes, w_final.T, w_out, att_near, att_far)
    theirs = swap(send_v, "guide")
    flat = near * channels
    own, odd, two, even = call(
        spread_kernel,
        [
            ((flat, 2 * columns), f32), ((flat, 2 * columns), bf16),
            ((flat, 2 * columns), bf16), ((flat, 2 * columns), bf16),
        ],
        smem=(0,), count=5, limit=8,
    )(scalars, facts, mine_v, theirs, latent)
    ups = [(i, (i + 1) % width) for i in range(width)]
    turns = [[pair for pair in ups if pair[0] % 2 == side] for side in range(2)]
    turns = [pairs + [(b, a) for a, b in pairs] for pairs in turns]
    odd = lax.ppermute(odd, "width", turns[1])
    two = lax.ppermute(two, "width", [(i, (i + 2) % width) for i in range(width)])
    even = lax.ppermute(even, "width", turns[0])
    return call(
        functools.partial(decode_kernel, width=width),
        [((channels, height // 2, columns), f32), ((height // 2, columns, w_dec.shape[1]), bf16)],
        scratch=[
            pltpu.VMEM((3, near + 2, channels, columns), f32),
        ],
        smem=(0, 1), count=9, limit=8,
    )(scalars, step_index, own, odd, two, even, latent, counts[None], w_dec)


def solution(mesh):
    return jax.shard_map(
        shards,
        mesh=mesh,
        in_specs=(
            P(None, None, ("groups", "width")),
            P(("groups", "width")),
            P(("groups", "width")),
            P("groups"),
            P("guide", None, None),
            P(),
            P("width", None),
            P(),
            P(),
            P(),
        ),
        out_specs=(P(None, "guide", ("groups", "width")), P("guide", ("groups", "width"), None)),
        check_vma=False,
    )
```
